512 devices in a mesh: seq: 64 (over y, z_hi, core), tp: 8 (over x, z_lo).
Axes of the slice: x: 4, y: 8, z: 8 (z_hi: 4, z_lo: 2; z = z_hi * 2 + z_lo), core: 2. Of those that a mesh axis runs over, the one named last changes fastest.
Arguments:
- rollout_rows: bfloat16 [24576, 5120], P('seq', 'tp'), may hold values from -6 to 6
- live_rows: int32 [64], P('seq'), may hold values from 129 to 383, as said below
- doc_lengths: int32 [32], replicated, may hold values from 1 to 769, 16384 in all
- block_owner: int32 [64], replicated, may hold values from 0 to 63, each once
- norm_gain: bfloat16 [5120], replicated, may hold values from 0.099609375 to 1.8984375
- qkv_weight: bfloat16 [5120, 5120], P('seq', 'tp'), may hold values from -1.8168052 to 1.8168052
- out_weight: bfloat16 [5120, 3072], P('seq', 'tp'), may hold values from -0.109375 to 0.109375
Outputs:
- layer_out: bfloat16 [16384, 5120], P('seq', 'tp')
- key_cache: bfloat16 [16384, 1024], P('seq', 'tp')
- value_cache: bfloat16 [16384, 1024], P('seq', 'tp')
The draws below stay inside these ranges and needn't reach their ends.
Inputs may be any that keep to these rules, and one draw needn't show every extreme that they name: Device s's live rows number live_rows[s]; the live rows of the devices before s number at least 256 * s and less than 256 * s + 128; all live rows together number 16384. `block_owner`: a permutation.
All inputs are finite; a program needn't handle non-finite values.
Results may differ from the reference program's by a relative error of at most 0.015.
The reference program's roundings to bfloat16 on the way count: a program that leaves them out, or rounds other values in their place, can miss the bound.
Values may be sent and summed in bfloat16 or wider, within the bound.
A program may use at most 64 MiB of HBM per device.

```python
import math
import jax
import jax.numpy as jnp
import numpy as np
from jax import lax

D = 5120
KV_HEADS = 8
HD = 128
HEADS = 24
WINDOW = 4
TOK_DEV = 256
CAP = 384
TOKENS = 16384
DOCS = 32
MOST = 769
QKV_COLS = 5120
N_SEQ = 64
N_TP = 8


def draw_live_rows(key, part):
    half_rows = TOK_DEV // 2
    first_key, second_key = jax.random.split(jax.random.fold_in(key, 11))
    spilled = jax.random.randint(first_key, (N_SEQ,), 0, half_rows)
    chosen = jax.random.randint(second_key, (), 1, N_SEQ - 1)
    indices = jnp.arange(N_SEQ)
    spilled = jnp.where(indices == chosen, half_rows - 1, spilled)
    spilled = jnp.where(indices == chosen - 1, 0, spilled)
    spilled = jnp.where(indices == chosen + 1, 0, spilled)
    spilled = jnp.where(indices == N_SEQ - 1, 0, spilled)
    earlier = jnp.concatenate([jnp.zeros((1,), spilled.dtype), spilled[:-1]])
    return (TOK_DEV + spilled - earlier).astype(jnp.int32)


def draw_qkv_weight(key, part):
    base_key = jax.random.fold_in(jax.random.fold_in(key, 21), 0)
    base = jax.random.truncated_normal(base_key, -4.0, 4.0, (D, QKV_COLS), jnp.float32) * D ** (-0.5)
    return base.astype(jnp.bfloat16)


def levels(rng, dims, shards, smallest, largest):
    def one(dim, blocks):
        draws = jax.random.uniform(jax.random.fold_in(jax.random.fold_in(rng, 6), dim), (blocks,), jnp.float32, smallest / len(shards), largest / len(shards))
        return jnp.repeat(jnp.exp(draws), dims[dim] // blocks).reshape((-1,) + (1,) * (len(dims) - dim - 1))

    gain = one(*shards[0])
    for cut in shards[1:]:
        gain = gain * one(*cut)
    return gain


def split_up(number_of, total, most, slope):
    portions = [(1 << 20) // math.isqrt(grade ** slope) + 1 for grade in range(2, number_of + 1)]
    spare, counts = total - most - (number_of - 1), [1] * (number_of - 1)
    while spare > 0:
        free = [i for i in range(number_of - 1) if counts[i] < most]
        whole, left = sum([portions[i] for i in free]), spare
        for i in free:
            addition = min(most - counts[i], max(1, left * portions[i] // whole), spare)
            counts[i] = counts[i] + addition
            spare = spare - addition
    return np.array([most] + counts)


def ragged_sizes(stream_key, amount, total, reach, slope):
    if amount == 2:
        one = jax.random.randint(stream_key, (), max(1, total - reach), min(reach, total - 1) + 1)
        return jnp.stack([one, total - one])
    tallies = jnp.asarray(split_up(amount, total, reach, slope), jnp.int32)
    couples = (amount - 1) // 2
    source_of, sink = tallies[1:1 + 2 * couples:2], tallies[2:2 + 2 * couples:2]
    room = jnp.minimum(source_of - 1, reach - sink)
    passed = jax.random.randint(jax.random.fold_in(stream_key, 1), (couples,), 0, 1 << 20) % (room + 1)
    tallies = tallies.at[1:1 + 2 * couples:2].set(source_of - passed).at[2:2 + 2 * couples:2].set(sink + passed)
    return tallies[jax.random.permutation(jax.random.fold_in(stream_key, 2), amount)]


def noise(rng, extent, scale, limit, pieces=(), held_as=jnp.bfloat16):
    result = jax.random.normal(rng, extent, jnp.float32) * scale
    if len(pieces) > 0:
        result = levels(rng, extent, pieces, -0.22, 0.18) * result
    return jnp.clip(result, min=-limit, max=limit).astype(held_as)


def setup_inputs(seed: int = 0) -> dict:
    arg_keys = jax.random.split(jax.random.key(seed), 8)
    rollout_rows = noise(arg_keys[0], (N_SEQ * CAP, D), 1.0, 6.0, ((0, 64), (1, 8)))
    live_rows = draw_live_rows(jax.random.fold_in(arg_keys[7], 71), 0)
    doc_lengths = ragged_sizes(arg_keys[2], DOCS, TOKENS, MOST, 2).astype(jnp.int32)
    block_owner = jax.random.permutation(arg_keys[3], N_SEQ).astype(jnp.int32)
    norm_gain = jnp.clip(1.0 + 0.18 * jax.random.normal(arg_keys[4], (D,), jnp.float32), 0.099609375, 1.8984375).astype(jnp.bfloat16)
    qkv_weight = draw_qkv_weight(jax.random.fold_in(arg_keys[7], 71), 0)
    out_weight = noise(arg_keys[6], (D, HEADS * HD), (HEADS * HD) ** -0.5, 0.109375, ((0, 64), (1, 8)))
    return {"rollout_rows": rollout_rows, "live_rows": live_rows, "doc_lengths": doc_lengths, "block_owner": block_owner, "norm_gain": norm_gain, "qkv_weight": qkv_weight, "out_weight": out_weight}


EPSILON = 1e-06
NEG_LARGE = -1e+30

def reference(rollout_rows, live_rows, doc_lengths, block_owner, norm_gain, qkv_weight, out_weight):
    offsets = jnp.cumsum(live_rows) - live_rows
    position = jnp.arange(TOKENS, dtype=jnp.int32)
    source = lax.optimization_barrier(jnp.sum((offsets[None, 1:] <= position[:, None]).astype(jnp.int32), axis=1)).astype(jnp.int32)
    local_row = position - offsets[source]
    stream = rollout_rows[source * CAP + local_row]
    values_f = stream.astype(jnp.float32)
    scale = lax.rsqrt(lax.optimization_barrier(jnp.mean(values_f * values_f, axis=-1, keepdims=True)) + EPSILON)
    normed = (values_f * scale * norm_gain.astype(jnp.float32)).astype(jnp.bfloat16)
    block_rows = D // N_SEQ
    permuted = normed.reshape(TOKENS, N_SEQ, block_rows)[:, block_owner, :].reshape(TOKENS, D)
    projected = jnp.dot(permuted, qkv_weight, preferred_element_type=jnp.float32)
    group = HEADS // KV_HEADS
    kv_local = KV_HEADS // N_TP
    width = QKV_COLS // N_TP
    q_width = kv_local * group * HD
    cube = projected.reshape(TOKENS, N_TP, width)
    query = (cube[:, :, :q_width] * HD ** (-0.5)).astype(jnp.bfloat16).reshape(TOKENS, KV_HEADS, group, HD)
    key_all = cube[:, :, q_width:q_width + kv_local * HD].astype(jnp.bfloat16).reshape(TOKENS, KV_HEADS, HD)
    value_all = cube[:, :, q_width + kv_local * HD:].astype(jnp.bfloat16).reshape(TOKENS, KV_HEADS, HD)
    doc_starts = jnp.cumsum(doc_lengths) - doc_lengths
    first_pos = lax.optimization_barrier(jnp.max(jnp.where(doc_starts[None, :] <= position[:, None], doc_starts[None, :], 0), axis=1))
    padding = (WINDOW - 1) * TOK_DEV
    key_pad = jnp.concatenate([jnp.zeros((padding, KV_HEADS, HD), jnp.bfloat16), key_all], 0)
    value_pad = jnp.concatenate([jnp.zeros((padding, KV_HEADS, HD), jnp.bfloat16), value_all], 0)

    def one_block(block):
        begin = (block * TOK_DEV).astype(jnp.int32)
        queries = lax.dynamic_slice_in_dim(query, begin, TOK_DEV, 0)
        keys_block = lax.dynamic_slice_in_dim(key_pad, begin, WINDOW * TOK_DEV, 0)
        values_block = lax.dynamic_slice_in_dim(value_pad, begin, WINDOW * TOK_DEV, 0)
        query_pos = begin + jnp.arange(TOK_DEV, dtype=jnp.int32)
        key_pos = begin - padding + jnp.arange(WINDOW * TOK_DEV, dtype=jnp.int32)
        starts = lax.dynamic_slice_in_dim(first_pos, begin, TOK_DEV, 0)
        allowed = (key_pos[None, :] <= query_pos[:, None]) & (key_pos[None, :] >= starts[:, None])
        scores = jnp.einsum('tgjd,sgd->gjts', queries.astype(jnp.float32), keys_block.astype(jnp.float32))
        masked = jnp.where(allowed, scores, NEG_LARGE)
        highest = lax.optimization_barrier(jnp.max(masked, axis=-1, keepdims=True))
        expo = jnp.where(allowed, jnp.exp(masked - highest), 0.0)
        totals = lax.optimization_barrier(jnp.sum(expo, axis=-1))
        summed = jnp.einsum('gjts,sgd->tgjd', expo.astype(jnp.bfloat16).astype(jnp.float32), values_block.astype(jnp.float32))
        context = summed / jnp.transpose(totals, (2, 0, 1))[..., None]
        return context.astype(jnp.bfloat16).reshape(TOK_DEV, HEADS * HD)
    context_all = lax.map(one_block, jnp.arange(N_SEQ, dtype=jnp.int32)).reshape(TOKENS, HEADS * HD)
    head_width = HEADS * HD // N_TP
    context_groups = context_all.reshape(TOKENS, N_TP, head_width)
    weight_groups = out_weight.reshape(D, N_TP, head_width)
    summed_out = jnp.zeros((TOKENS, D), jnp.float32)
    for group_index in range(N_TP):
        partial_value = lax.dot_general(context_groups[:, group_index, :], weight_groups[:, group_index, :], (((1,), (1,)), ((), ())), preferred_element_type=jnp.float32)
        rounded = lax.optimization_barrier(partial_value.astype(jnp.bfloat16))
        summed_out = summed_out + rounded.astype(jnp.float32)
    placed = jnp.zeros((TOKENS, N_SEQ, block_rows), jnp.float32).at[:, block_owner, :].set(summed_out.reshape(TOKENS, N_SEQ, block_rows))
    layer_out = placed.reshape(TOKENS, D).astype(jnp.bfloat16)
    return (layer_out, key_all.reshape(TOKENS, KV_HEADS * HD), value_all.reshape(TOKENS, KV_HEADS * HD))
```

```python
import jax
import jax.numpy as jnp
from jax import lax
from jax.experimental import pallas as pl
from jax.experimental.pallas import tpu as pltpu
from jax.sharding import PartitionSpec as P

D = 5120
HD = 128
GROUP = 3
TOK = 256
HALF = 128
CAP = 384
BLK = 80
N_SEQ = 64
N_TP = 8
N_Y, N_Z, N_X = 8, 4, 4
COLS = 640
QW = GROUP * HD
EPSILON = 1e-06
NEG = -1e30
N_COPIES = 176
MESH = pl.DeviceIdType.MESH
BF = jnp.bfloat16
F32 = jnp.float32


def kernel(
    live_s, docs_s, slot_s, gain_v, roll_h, wq_h, wo_h,
    out_ref, key_ref, value_ref,
    rows, wq, wo, acts, tail_s, tail_r, live_own, live_p, live_z, live_y, ssq,
    acc, kv_own, kv_in, bias, ctx, part_s, part_r,
    local_sem, send_sem, recv_sem,
):
    seq = lax.axis_index("seq")
    tp = lax.axis_index("tp")
    core = lax.rem(seq, 2)
    zh = lax.rem(lax.div(seq, 2), N_Z)
    y = lax.div(seq, 2 * N_Z)
    zl = lax.rem(tp, 2)
    x = lax.div(tp, 2)
    d = 1 - 2 * core

    def wrap_y(v):
        return lax.rem(v + 2 * N_Y, N_Y)

    def wrap_z(v):
        return lax.rem(v + 2 * N_Z, N_Z)

    def wrap_x(v):
        return lax.rem(v + 2 * N_X, N_X)

    def at_seq(y_, z_, c_):
        return ((y_ * N_Z + z_) * 2 + c_, tp)

    def at_tp(x_, zl_):
        return (seq, x_ * 2 + zl_)

    def slot(y_, z_):
        return core * (N_Y * N_Z) + y_ * N_Z + z_

    partner = at_seq(y, zh, 1 - core)
    next_1 = (lax.rem(seq + 1, N_SEQ), tp)
    next_2 = (lax.rem(seq + 2, N_SEQ), tp)
    prev_1 = (lax.rem(seq + N_SEQ - 1, N_SEQ), tp)
    prev_2 = (lax.rem(seq + N_SEQ - 2, N_SEQ), tp)

    started = []

    def send(src, dst, device):
        n = len(started)
        copy = pltpu.make_async_remote_copy(
            src_ref=src, dst_ref=dst, send_sem=send_sem.at[n], recv_sem=recv_sem.at[n],
            device_id=device, device_id_type=MESH,
        )
        copy.start()
        started.append(copy)
        return copy

    load_q = pltpu.make_async_copy(wq_h, wq.at[slot(y, zh)], local_sem.at[0])
    load_o = pltpu.make_async_copy(wo_h, wo.at[slot(y, zh)], local_sem.at[1])
    load_r = pltpu.make_async_copy(roll_h, rows, local_sem.at[2])
    load_q.start()
    load_r.start()
    load_o.start()

    barrier = pltpu.get_barrier_semaphore()
    greeted = [partner, next_1, next_2, prev_1, prev_2]
    greeted += [at_seq(y, wrap_z(zh + k), core) for k in range(1, N_Z)]
    greeted += [at_seq(wrap_y(y + k), zh, core) for k in range(1, N_Y)]
    greeted += [(seq, lax.rem(tp + k, N_TP)) for k in range(1, N_TP)]
    for device in greeted:
        pl.semaphore_signal(barrier, inc=1, device_id=device, device_id_type=MESH)
    live_own[...] = jnp.full((8, 128), live_s[0], jnp.int32)
    gain_rows = gain_v[...].astype(F32)
    picked = lax.broadcasted_iota(jnp.int32, (N_TP, COLS), 0) == tp
    gain = jnp.sum(jnp.where(picked, gain_rows, 0.0), axis=0, keepdims=True)
    load_q.wait()
    load_r.wait()
    pl.semaphore_wait(barrier, len(greeted))

    up_z = at_seq(y, wrap_z(zh + d), core)
    down_z = at_seq(y, wrap_z(zh - d), core)
    up_y = at_seq(wrap_y(y + d), zh, core)
    down_y = at_seq(wrap_y(y - d), zh, core)

    def z_own(buf):
        own = buf.at[slot(y, zh)]
        return send(own, own, up_z), send(own, own, down_z)

    def z_on(buf):
        held = buf.at[slot(y, wrap_z(zh - d))]
        return send(held, held, up_z)

    z_blocks = [zh, wrap_z(zh - d), wrap_z(zh + d), wrap_z(zh + 2 * d)]

    def ring_up(buf, b, k):
        held = buf.at[slot(wrap_y(y - (k - 1) * d), z_blocks[b])]
        return send(held, held, up_y)

    def ring_down(buf, b, k):
        held = buf.at[slot(wrap_y(y + (k - 1) * d), z_blocks[b])]
        return send(held, held, down_y)

    def across(buf, k):
        held = buf.at[pl.ds(core * (N_Y * N_Z) + wrap_y(y + k * d) * N_Z, N_Z)]
        return send(held, held, partner)

    q_up, q_down = {}, {}
    q_z1, q_z2 = z_own(wq)
    q_up[0, 1], q_down[0, 1] = ring_up(wq, 0, 1), ring_down(wq, 0, 1)

    live_to_partner = send(live_own, live_p, partner)

    def squares(values):
        total = jnp.sum(values * values, axis=1, keepdims=True)
        return jnp.transpose(jnp.broadcast_to(total, (HALF, 128)))[:8]

    own_a = rows[pl.ds(0, HALF), :].astype(F32)
    acts[tp, pl.ds(0, HALF), :] = (own_a * gain).astype(BF)
    x_up = at_tp(wrap_x(x + 1), zl)
    x_down = at_tp(wrap_x(x - 1), zl)
    z_other = at_tp(x, 1 - zl)

    def chunk(x_, zl_, part):
        return acts.at[wrap_x(x_) * 2 + zl_, pl.ds(part * HALF, HALF)]

    def gather_own(part):
        own = chunk(x, zl, part)
        return [send(own, own, z_other), send(own, own, x_up), send(own, own, x_down)]

    def gather_second(part):
        held = chunk(x, 1 - zl, part)
        return [send(held, held, x_up), send(held, held, x_down)]

    def gather_third_up(part):
        held = chunk(x - 1, zl, part)
        return send(held, held, x_up)

    def gather_third_down(part):
        held = chunk(x + 1, 1 - zl, part)
        return send(held, held, x_down)

    a_first = gather_own(0)

    row = lax.broadcasted_iota(jnp.int32, (HALF, CAP), 0)
    col = lax.broadcasted_iota(jnp.int32, (HALF, CAP), 1)
    chosen = (col == row + (live_s[0] - HALF)).astype(BF)
    tail_s[...] = jnp.dot(chosen, rows[...], preferred_element_type=F32).astype(BF)
    tail = send(tail_s, tail_r, next_1)

    ssq[tp, 0] = squares(own_a)

    live_to_partner.wait_recv()
    live_z[0] = live_own[...] + live_p[...]
    live_over_z = [
        send(live_z.at[0], live_z.at[k], at_seq(y, wrap_z(zh + k), core)) for k in range(1, N_Z)
    ]

    position = seq * TOK + lax.broadcasted_iota(jnp.int32, (TOK, 128), 0)
    first = jnp.zeros((TOK, 128), jnp.int32)
    begin = docs_s[0]
    for doc in range(1, 32):
        first = jnp.maximum(first, jnp.where(position >= begin, begin, 0))
        begin = begin + docs_s[doc]
    key_base = [seq, seq - 2, seq - 3 + 2 * core, seq - 1 - 2 * core]
    lane = lax.broadcasted_iota(jnp.int32, (TOK, 128), 1)
    for b in range(4):
        for side in range(2):
            key_pos = key_base[b] * TOK + side * 128 + lane
            allowed = (key_pos <= position) & (key_pos >= first)
            bias[b, :, pl.ds(side * 128, 128)] = jnp.where(allowed, 0.0, NEG)

    q_z1.wait_recv()
    q_z3 = z_on(wq)
    q_up[1, 1], q_down[1, 1] = ring_up(wq, 1, 1), ring_down(wq, 1, 1)
    q_z2.wait_recv()
    q_up[2, 1], q_down[2, 1] = ring_up(wq, 2, 1), ring_down(wq, 2, 1)
    a_first[0].wait_recv()
    a_second = gather_second(0)
    for copy in live_over_z:
        copy.wait_recv()
    live_y[0] = live_z[0] + live_z[1] + live_z[2] + live_z[3]
    live_over_y = [
        send(live_y.at[0], live_y.at[k], at_seq(wrap_y(y + k), zh, core)) for k in range(1, N_Y)
    ]
    q_z3.wait_recv()
    q_up[3, 1], q_down[3, 1] = ring_up(wq, 3, 1), ring_down(wq, 3, 1)
    q_across = [across(wq, 0)]
    a_first[1].wait_recv()
    a_third = [gather_third_up(0)]
    a_second[1].wait_recv()
    a_third.append(gather_third_down(0))

    for copy in live_over_y:
        copy.wait_recv()
    before = live_p[...] * core - seq * TOK
    for k in range(1, N_Z):
        before = before + live_z[k] * (k <= zh).astype(jnp.int32)
    for k in range(1, N_Y):
        before = before + live_y[k] * (k <= y).astype(jnp.int32)
    spilled = before[:1, :]
    tail.wait_recv()
    row_b = lax.broadcasted_iota(jnp.int32, (HALF, 128), 0)
    keep = jnp.broadcast_to((row_b + spilled < HALF)[:, :1], (HALF, COLS))
    own_b = jnp.where(
        keep, rows[pl.ds(HALF, HALF), :].astype(F32), tail_r[...].astype(F32)
    )
    acts[tp, pl.ds(HALF, HALF), :] = (own_b * gain).astype(BF)
    b_first = gather_own(1)
    ssq[tp, 1] = squares(own_b)
    ssq_copies = [
        send(ssq.at[tp], ssq.at[tp], (seq, lax.rem(tp + k, N_TP))) for k in range(1, N_TP)
    ]

    load_o.wait()
    o_up, o_down = {}, {}
    o_z1, o_z2 = z_own(wo)

    def step(buf, up, down, k):
        for b in range(4):
            up[b, k - 1].wait_recv()
            up[b, k] = ring_up(buf, b, k)
            down[b, k - 1].wait_recv()
            if k < 4:
                down[b, k] = ring_down(buf, b, k)
        return [across(buf, -(k - 1)), across(buf, k - 1)]

    q_across += step(wq, q_up, q_down, 2)
    b_first[0].wait_recv()
    b_second = gather_second(1)
    o_z1.wait_recv()
    o_z3 = z_on(wo)
    b_first[1].wait_recv()
    b_third = [gather_third_up(1)]
    b_second[1].wait_recv()
    b_third.append(gather_third_down(1))
    q_across += step(wq, q_up, q_down, 3)
    q_across += step(wq, q_up, q_down, 4)

    o_z2.wait_recv()
    o_z3.wait_recv()
    for b in range(4):
        o_up[b, 1], o_down[b, 1] = ring_up(wo, b, 1), ring_down(wo, b, 1)
    o_across = [across(wo, 0)]

    for b in range(4):
        q_up[b, 4].wait_recv()
    q_across.append(across(wq, 4))
    for copy in a_first[2:] + a_second[:1] + a_third + b_first[2:] + b_second[:1] + b_third:
        copy.wait_recv()
    for copy in ssq_copies:
        copy.wait_recv()
    for copy in q_across:
        copy.wait_recv()

    acc[...] = jnp.zeros_like(acc)

    def project(t, carry):
        blocks = [wq[slot_s[t * 8 + i]] for i in range(8)]
        weight = jnp.concatenate(blocks, axis=0)
        acc[...] += jnp.dot(acts[t], weight, preferred_element_type=F32)
        return carry

    lax.fori_loop(0, N_TP, project, 0)
    o_across += step(wo, o_up, o_down, 2)

    total = ssq[0]
    for t in range(1, N_TP):
        total = total + ssq[t]
    scale_row = lax.rsqrt(total * (1.0 / D) + EPSILON)
    scale = jnp.concatenate(
        [jnp.transpose(jnp.broadcast_to(scale_row[h, :1], (128, 128))) for h in range(2)], axis=0
    )
    turn_row = lax.broadcasted_iota(jnp.int32, (TOK, TOK), 0)
    turn_col = lax.broadcasted_iota(jnp.int32, (TOK, TOK), 1)
    spilled_wide = jnp.concatenate([spilled, spilled], axis=1)
    turn = (((turn_col - turn_row + spilled_wide + TOK) & (TOK - 1)) == 0).astype(BF)

    def in_order(values):
        return jnp.dot(turn, values, preferred_element_type=F32).astype(BF)

    keys = in_order((acc[:, QW : QW + HD] * scale).astype(BF))
    values = in_order((acc[:, QW + HD :] * scale).astype(BF))
    kv_own[:, :HD] = keys
    kv_own[:, HD:] = values
    kv_1 = send(kv_own, kv_in.at[0], next_2)
    n_kv = len(started)

    def kv_copy(src):
        return pltpu.make_async_remote_copy(
            src_ref=src, dst_ref=kv_in.at[1], send_sem=send_sem.at[n_kv],
            recv_sem=recv_sem.at[n_kv], device_id=next_1, device_id_type=MESH,
        )

    @pl.when(core == 0)
    def _():
        kv_copy(kv_own).start()

    kv_2 = kv_copy(kv_own)
    started.append(kv_2)
    key_ref[...] = keys
    value_ref[...] = values
    queries = [
        in_order((acc[:, h * HD : (h + 1) * HD] * scale * HD ** (-0.5)).astype(BF))
        for h in range(GROUP)
    ]
    kv_1.wait_recv()

    @pl.when(core == 1)
    def _():
        kv_copy(kv_in.at[0]).start()

    kv_3 = send(kv_in.at[0], kv_in.at[2], partner)
    o_across += step(wo, o_up, o_down, 3)
    kv_2.wait_recv()
    kv_3.wait_recv()
    o_across += step(wo, o_up, o_down, 4)

    pieces = [kv_own, kv_in.at[0], kv_in.at[1], kv_in.at[2]]
    for h in range(GROUP):
        scores = [
            lax.dot_general(
                queries[h], pieces[b][:, :HD], (((1,), (1,)), ((), ())),
                preferred_element_type=F32,
            ) + bias[b]
            for b in range(4)
        ]
        best = jnp.maximum(
            jnp.maximum(scores[0], scores[1]), jnp.maximum(scores[2], scores[3])
        )
        best = jnp.max(best, axis=1, keepdims=True)
        weights = [jnp.exp(s - best) for s in scores]
        totals = jnp.sum(weights[0] + weights[1] + weights[2] + weights[3], axis=1, keepdims=True)
        summed = jnp.dot(weights[0].astype(BF), pieces[0][:, HD:], preferred_element_type=F32)
        for b in range(1, 4):
            summed = summed + jnp.dot(
                weights[b].astype(BF), pieces[b][:, HD:], preferred_element_type=F32
            )
        ctx[:, h * HD : (h + 1) * HD] = (summed / totals).astype(BF)

    for b in range(4):
        o_up[b, 4].wait_recv()
    o_across.append(across(wo, 4))
    for copy in o_across:
        copy.wait_recv()

    base = len(started)

    def partial_sum(t):
        weight = jnp.concatenate([wo[slot_s[t * 8 + i]] for i in range(8)], axis=0)
        delivered = lax.dot_general(
            ctx[...], weight, (((1,), (1,)), ((), ())), preferred_element_type=F32
        )
        return delivered.astype(BF)

    def part_copy(k):
        t = lax.rem(tp + k, N_TP)
        return pltpu.make_async_remote_copy(
            src_ref=part_s.at[k], dst_ref=part_r.at[k], send_sem=send_sem.at[base + k - 1],
            recv_sem=recv_sem.at[base + k - 1], device_id=(seq, t), device_id_type=MESH,
        )

    def deliver(i, carry):
        k = lax.rem(i + 4, N_TP)
        t = lax.rem(tp + k, N_TP)
        part_s[k] = partial_sum(t)

        @pl.when(k > 0)
        def _():
            part_copy(k).start()

        return carry

    lax.fori_loop(0, N_TP, deliver, 0)

    mixed = part_s[0].astype(F32)
    for k in range(1, N_TP):
        part_copy(k).wait_recv()
        mixed = mixed + part_r[k].astype(F32)
    out_ref[...] = mixed.astype(BF)
    for copy in started:
        copy.wait_send()
    for k in range(1, N_TP):
        part_copy(k).wait_send()


def body(rollout_rows, live_rows, doc_lengths, block_owner, norm_gain, qkv_weight, out_weight):
    positions = jnp.arange(N_SEQ, dtype=jnp.int32)
    slots = lax.rem(positions, 2) * (N_SEQ // 2) + positions // 2
    slot_of = jnp.sum(
        jnp.where(block_owner[None, :] == positions[:, None], slots[None, :], 0), axis=1
    )
    smem = pl.BlockSpec(memory_space=pltpu.SMEM)
    vmem = pl.BlockSpec(memory_space=pltpu.VMEM)
    anyw = pl.BlockSpec(memory_space=pl.ANY)
    V = pltpu.VMEM
    return pl.pallas_call(
        kernel,
        out_shape=(
            jax.ShapeDtypeStruct((TOK, COLS), BF),
            jax.ShapeDtypeStruct((TOK, HD), BF),
            jax.ShapeDtypeStruct((TOK, HD), BF),
        ),
        in_specs=[smem, smem, smem, vmem, anyw, anyw, anyw],
        out_specs=(vmem, vmem, vmem),
        scratch_shapes=[
            V((CAP, COLS), BF),
            V((N_SEQ, BLK, COLS), BF),
            V((N_SEQ, BLK, QW), BF),
            V((N_TP, TOK, COLS), BF),
            V((HALF, COLS), BF),
            V((HALF, COLS), BF),
            V((8, 128), jnp.int32),
            V((8, 128), jnp.int32),
            V((N_Z, 8, 128), jnp.int32),
            V((N_Y, 8, 128), jnp.int32),
            V((N_TP, 2, 8, 128), F32),
            V((TOK, COLS), F32),
            V((TOK, 2 * HD), BF),
            V((3, TOK, 2 * HD), BF),
            V((4, TOK, TOK), F32),
            V((TOK, QW), BF),
            V((N_TP, TOK, COLS), BF),
            V((N_TP, TOK, COLS), BF),
            pltpu.SemaphoreType.DMA((3,)),
            pltpu.SemaphoreType.DMA((N_COPIES,)),
            pltpu.SemaphoreType.DMA((N_COPIES,)),
        ],
        compiler_params=pltpu.CompilerParams(collective_id=0, has_side_effects=True),
    )(
        live_rows, doc_lengths, slot_of, norm_gain.reshape(N_TP, COLS),
        rollout_rows, qkv_weight, out_weight,
    )


def solution(mesh):
    in_specs = (P("seq", "tp"), P("seq"), P(), P(), P(), P("seq", "tp"), P("seq", "tp"))
    out_specs = (P("seq", "tp"), P("seq", "tp"), P("seq", "tp"))
    return jax.shard_map(body, mesh=mesh, in_specs=in_specs, out_specs=out_specs, check_vma=False)
```

```python
import jax
import jax.numpy as jnp
from jax import lax
from jax.experimental import pallas as pl
from jax.experimental.pallas import tpu as pltpu
from jax.sharding import PartitionSpec as P

D = 5120
HD = 128
GROUP = 3
TOK = 256
HALF = 128
CAP = 384
BLK = 80
N_SEQ = 64
N_TP = 8
N_Y, N_Z, N_X = 8, 4, 4
COLS = 640
QW = GROUP * HD
EPSILON = 1e-06
NEG = -1e30
N_COPIES = 200
O_FIRST = 48
R1 = 112
MESH = pl.DeviceIdType.MESH
BF = jnp.bfloat16
F32 = jnp.float32


def kernel(
    live_s, docs_s, slot_s, gain_v, roll_h, wqkv_h, wo_h,
    out_ref, key_ref, value_ref,
    rows, wkv, wq, wo, acts, tail_s, tail_r, live_own, live_p, live_z, live_y, ssq,
    acc_kv, acc_q, kv_own, kv_in, bias, ctx, part,
    z1_r, pair_s, x1_r, x2_r, sum2_s, z2_s, z2_r,
    local_sem, send_sem, recv_sem,
):
    seq = lax.axis_index("seq")
    tp = lax.axis_index("tp")
    core = lax.rem(seq, 2)
    zh = lax.rem(lax.div(seq, 2), N_Z)
    y = lax.div(seq, 2 * N_Z)
    zl = lax.rem(tp, 2)
    x = lax.div(tp, 2)
    d = 1 - 2 * core

    def wrap_y(v):
        return lax.rem(v + 2 * N_Y, N_Y)

    def wrap_z(v):
        return lax.rem(v + 2 * N_Z, N_Z)

    def wrap_x(v):
        return lax.rem(v + 2 * N_X, N_X)

    def at_seq(y_, z_, c_):
        return ((y_ * N_Z + z_) * 2 + c_, tp)

    def at_tp(x_, zl_):
        return (seq, x_ * 2 + zl_)

    partner = at_seq(y, zh, 1 - core)
    next_1 = (lax.rem(seq + 1, N_SEQ), tp)
    next_2 = (lax.rem(seq + 2, N_SEQ), tp)
    prev_1 = (lax.rem(seq + N_SEQ - 1, N_SEQ), tp)
    prev_2 = (lax.rem(seq + N_SEQ - 2, N_SEQ), tp)

    started = []

    def send(src, dst, device):
        n = len(started)
        copy = pltpu.make_async_remote_copy(
            src_ref=src, dst_ref=dst, send_sem=send_sem.at[n], recv_sem=recv_sem.at[n],
            device_id=device, device_id_type=MESH,
        )
        copy.start()
        started.append(copy)
        return copy

    loads = [
        pltpu.make_async_copy(wqkv_h.at[:, pl.ds(QW, 2 * HD)], wkv.at[core, y, zh], local_sem.at[0]),
        pltpu.make_async_copy(wqkv_h.at[:, pl.ds(0, QW)], wq.at[core, y, zh], local_sem.at[1]),
        pltpu.make_async_copy(roll_h, rows, local_sem.at[2]),
        pltpu.make_async_copy(wo_h, wo.at[core, y, zh], local_sem.at[3]),
    ]
    for load in loads:
        load.start()

    barrier = pltpu.get_barrier_semaphore()
    greeted = [partner, next_1, next_2, prev_1, prev_2]
    greeted += [at_seq(y, wrap_z(zh + k), core) for k in range(1, N_Z)]
    greeted += [at_seq(wrap_y(y + k), zh, core) for k in range(1, N_Y)]
    greeted += [(seq, lax.rem(tp + k, N_TP)) for k in range(1, N_TP)]
    for device in greeted:
        pl.semaphore_signal(barrier, inc=1, device_id=device, device_id_type=MESH)
    live_own[...] = jnp.full((8, 128), live_s[0], jnp.int32)
    gain_all = gain_v[...].astype(F32)
    gain_row = lax.broadcasted_iota(jnp.int32, (D // 128, 128), 0)
    gain = jnp.concatenate(
        [
            jnp.sum(jnp.where(gain_row == tp * 5 + i, gain_all, 0.0), axis=0, keepdims=True)
            for i in range(5)
        ],
        axis=1,
    )
    for load in loads:
        load.wait()
    own_a = rows[pl.ds(0, HALF), :].astype(F32)
    acts[tp, pl.ds(0, HALF), :] = (own_a * gain).astype(BF)
    pl.semaphore_wait(barrier, len(greeted))

    up_z = at_seq(y, wrap_z(zh + d), core)
    down_z = at_seq(y, wrap_z(zh - d), core)
    up_y = at_seq(wrap_y(y + d), zh, core)
    down_y = at_seq(wrap_y(y - d), zh, core)
    z_blocks = [zh, wrap_z(zh - d), wrap_z(zh + d), wrap_z(zh + 2 * d)]

    class Gather:
        def __init__(self, buf, first, count):
            self.buf, self.first, self.count = buf, first, count
            self.up, self.down, self.across = {}, {}, []

        def block(self, y_, z_):
            whole = self.count == BLK
            return self.buf.at[core, y_, z_] if whole else (
                self.buf.at[core, y_, z_, pl.ds(self.first, self.count)])

        def line_y(self, y_):
            whole = self.count == BLK
            return self.buf.at[core, y_] if whole else (
                self.buf.at[core, y_, :, pl.ds(self.first, self.count)])

        def line_z(self, z_):
            return self.buf.at[core, :, z_, pl.ds(self.first, self.count)]

        def z_own(self):
            own = self.block(y, zh)
            self.z1, self.z2 = send(own, own, up_z), send(own, own, down_z)

        def z_on(self):
            self.z1.wait_recv()
            held = self.block(y, z_blocks[1])
            self.z3 = send(held, held, up_z)

        def ring(self, b, k):
            if k > 1:
                self.up[b, k - 1].wait_recv()
            held = self.block(wrap_y(y - (k - 1) * d), z_blocks[b])
            self.up[b, k] = send(held, held, up_y)
            if k > 1:
                self.down[b, k - 1].wait_recv()
            if k < 4:
                held = self.block(wrap_y(y + (k - 1) * d), z_blocks[b])
                self.down[b, k] = send(held, held, down_y)

        def step(self, k):
            for b in range(4):
                self.ring(b, k)
            for side in (-(k - 1), k - 1)[: min(k, 2)]:
                held = self.line_y(wrap_y(y + side * d))
                self.across.append(send(held, held, partner))

        def z_arrived(self):
            self.ring(1, 1)
            self.z2.wait_recv()
            self.ring(2, 1)
            self.z3.wait_recv()
            self.ring(3, 1)
            held = self.line_y(y)
            self.across.append(send(held, held, partner))

        def last(self):
            for b in range(4):
                self.up[b, 4].wait_recv()
            held = self.line_y(wrap_y(y + 4))
            self.across.append(send(held, held, partner))

        def column_own(self):
            own = self.line_z(zh)
            self.c1, self.c2 = send(own, own, up_z), send(own, own, down_z)
            self.across.append(send(own, own, partner))

        def column_on(self):
            self.c1.wait_recv()
            held = self.line_z(z_blocks[1])
            self.c3 = send(held, held, up_z)
            self.across.append(send(held, held, partner))

        def column_last(self):
            self.c2.wait_recv()
            held = self.line_z(z_blocks[2])
            self.across.append(send(held, held, partner))
            self.c3.wait_recv()
            held = self.line_z(z_blocks[3])
            self.across.append(send(held, held, partner))

        def wait(self):
            for copy in self.across:
                copy.wait_recv()

    kv = Gather(wkv, 0, BLK)
    qq = Gather(wq, 0, BLK)
    o1 = Gather(wo, 0, O_FIRST)
    o2 = Gather(wo, O_FIRST, BLK - O_FIRST)

    def squares(values):
        total = jnp.sum(values * values, axis=1, keepdims=True)
        return jnp.transpose(jnp.broadcast_to(total, (HALF, 128)))[:8]

    x_up = at_tp(wrap_x(x + 1), zl)
    x_down = at_tp(wrap_x(x - 1), zl)
    z_other = at_tp(x, 1 - zl)

    class Tokens:
        def __init__(self, part):
            self.part = part

        def chunk(self, x_, zl_):
            return acts.at[wrap_x(x_) * 2 + zl_, pl.ds(self.part * HALF, HALF)]

        def own(self):
            own = self.chunk(x, zl)
            self.a = [send(own, own, z_other), send(own, own, x_up), send(own, own, x_down)]

        def second(self):
            self.a[0].wait_recv()
            held = self.chunk(x, 1 - zl)
            self.b = [send(held, held, x_up), send(held, held, x_down)]

        def third(self):
            self.a[1].wait_recv()
            held = self.chunk(x - 1, zl)
            self.c = [send(held, held, x_up)]
            self.b[1].wait_recv()
            held = self.chunk(x + 1, 1 - zl)
            self.c.append(send(held, held, x_down))

        def wait(self):
            for copy in [self.a[2], self.b[0], *self.c]:
                copy.wait_recv()

    tok_a, tok_b = Tokens(0), Tokens(1)

    kv.z_own()
    kv.ring(0, 1)
    live_to_partner = send(live_own, live_p, partner)
    o2.ring(0, 1)
    tok_a.own()
    qq.z_own()
    qq.ring(0, 1)

    row = lax.broadcasted_iota(jnp.int32, (HALF, CAP), 0)
    col = lax.broadcasted_iota(jnp.int32, (HALF, CAP), 1)
    chosen = (col == row + (live_s[0] - HALF)).astype(BF)
    tail_s[...] = jnp.dot(chosen, rows[...], preferred_element_type=F32).astype(BF)
    tail = send(tail_s, tail_r, next_1)
    live_to_partner.wait_recv()
    live_z[0] = live_own[...] + live_p[...]
    live_over_z = [
        send(live_z.at[0], live_z.at[k], at_seq(y, wrap_z(zh + k), core)) for k in range(1, N_Z)
    ]
    ssq[tp, 0] = squares(own_a)

    kv.z_on()
    kv.z_arrived()
    o2.ring(0, 2)
    tok_a.second()
    for copy in live_over_z:
        copy.wait_recv()
    live_y[0] = live_z[0] + live_z[1] + live_z[2] + live_z[3]
    live_over_y = [
        send(live_y.at[0], live_y.at[k], at_seq(wrap_y(y + k), zh, core)) for k in range(1, N_Y)
    ]
    kv.step(2)
    o2.ring(0, 3)
    qq.z_on()
    tok_a.third()
    kv.step(3)
    o2.ring(0, 4)

    for copy in live_over_y:
        copy.wait_recv()
    before = live_p[...] * core - seq * TOK
    for k in range(1, N_Z):
        before = before + live_z[k] * (k <= zh).astype(jnp.int32)
    for k in range(1, N_Y):
        before = before + live_y[k] * (k <= y).astype(jnp.int32)
    spilled = before[:1, :]
    tail.wait_recv()
    row_b = lax.broadcasted_iota(jnp.int32, (HALF, 128), 0)
    keep = jnp.broadcast_to((row_b + spilled < HALF)[:, :1], (HALF, COLS))
    own_b = jnp.where(
        keep, rows[pl.ds(HALF, HALF), :].astype(F32), tail_r[...].astype(F32)
    )
    acts[tp, pl.ds(HALF, HALF), :] = (own_b * gain).astype(BF)
    tok_b.own()
    ssq[tp, 1] = squares(own_b)
    ssq_copies = [
        send(ssq.at[tp], ssq.at[tp], (seq, lax.rem(tp + k, N_TP))) for k in range(1, N_TP)
    ]
    kv.step(4)
    qq.z_arrived()
    tok_b.second()

    position = seq * TOK + lax.broadcasted_iota(jnp.int32, (TOK, 128), 0)
    first = jnp.zeros((TOK, 128), jnp.int32)
    begin = docs_s[0]
    for doc in range(1, 32):
        first = jnp.maximum(first, jnp.where(position >= begin, begin, 0))
        begin = begin + docs_s[doc]
    key_base = [seq, seq - 2, seq - 3 + 2 * core, seq - 1 - 2 * core]
    lane = lax.broadcasted_iota(jnp.int32, (TOK, 128), 1)
    for b in range(4):
        for side in range(2):
            key_pos = key_base[b] * TOK + side * 128 + lane
            allowed = (key_pos <= position) & (key_pos >= first)
            bias[b, :, pl.ds(side * 128, 128)] = jnp.where(allowed, 0.0, NEG)

    o2.up[0, 4].wait_recv()
    o2.column_own()
    kv.last()
    qq.step(2)
    tok_b.third()
    o1.z_own()
    qq.step(3)
    o2.column_on()

    def weight_of(buf, t):
        blocks = []
        for i in range(8):
            s = slot_s[t * 8 + i]
            blocks.append(
                buf[lax.div(s, N_Y * N_Z), lax.rem(lax.div(s, N_Z), N_Y), lax.rem(s, N_Z)]
            )
        return jnp.concatenate(blocks, axis=0)

    def project(buf, total):
        total[...] = jnp.zeros_like(total)

        def one(t, carry):
            total[...] += jnp.dot(acts[t], weight_of(buf, t), preferred_element_type=F32)
            return carry

        lax.fori_loop(0, N_TP, one, 0)

    tok_a.wait()
    tok_b.wait()
    for copy in ssq_copies:
        copy.wait_recv()
    kv.wait()
    project(wkv, acc_kv)

    total = ssq[0]
    for t in range(1, N_TP):
        total = total + ssq[t]
    scale_row = lax.rsqrt(total * (1.0 / D) + EPSILON)
    scale = jnp.concatenate(
        [jnp.transpose(jnp.broadcast_to(scale_row[h, :1], (128, 128))) for h in range(2)], axis=0
    )
    turn_row = lax.broadcasted_iota(jnp.int32, (TOK, TOK), 0)
    turn_col = lax.broadcasted_iota(jnp.int32, (TOK, TOK), 1)
    spilled_wide = jnp.concatenate([spilled, spilled], axis=1)
    turn = (((turn_col - turn_row + spilled_wide + TOK) & (TOK - 1)) == 0).astype(BF)

    def in_order(values):
        return jnp.dot(turn, values, preferred_element_type=F32).astype(BF)

    keys = in_order((acc_kv[:, :HD] * scale).astype(BF))
    values = in_order((acc_kv[:, HD:] * scale).astype(BF))
    kv_own[:, :HD] = keys
    kv_own[:, HD:] = values
    kv_1 = send(kv_own, kv_in.at[0], next_2)
    n_kv = len(started)

    def kv_copy(src):
        return pltpu.make_async_remote_copy(
            src_ref=src, dst_ref=kv_in.at[1], send_sem=send_sem.at[n_kv],
            recv_sem=recv_sem.at[n_kv], device_id=next_1, device_id_type=MESH,
        )

    @pl.when(core == 0)
    def _():
        kv_copy(kv_own).start()

    kv_2 = kv_copy(kv_own)
    started.append(kv_2)
    key_ref[...] = keys
    value_ref[...] = values
    qq.step(4)
    o1.z_on()
    o1.ring(0, 1)
    o1.z_arrived()
    kv_1.wait_recv()

    @pl.when(core == 1)
    def _():
        kv_copy(kv_in.at[0]).start()

    kv_3 = send(kv_in.at[0], kv_in.at[2], partner)
    o2.column_last()
    qq.last()
    o1.step(2)
    qq.wait()
    project(wq, acc_q)
    queries = [
        in_order((acc_q[:, h * HD : (h + 1) * HD] * scale * HD ** (-0.5)).astype(BF))
        for h in range(GROUP)
    ]
    o1.step(3)
    kv_2.wait_recv()
    kv_3.wait_recv()

    pieces = [kv_own, kv_in.at[0], kv_in.at[1], kv_in.at[2]]
    for h in range(GROUP):
        scores = [
            lax.dot_general(
                queries[h], pieces[b][:, :HD], (((1,), (1,)), ((), ())),
                preferred_element_type=F32,
            ) + bias[b]
            for b in range(4)
        ]
        best = jnp.maximum(
            jnp.maximum(scores[0], scores[1]), jnp.maximum(scores[2], scores[3])
        )
        best = jnp.max(best, axis=1, keepdims=True)
        weights = [jnp.exp(s - best) for s in scores]
        totals = jnp.sum(weights[0] + weights[1] + weights[2] + weights[3], axis=1, keepdims=True)
        summed = jnp.dot(weights[0].astype(BF), pieces[0][:, HD:], preferred_element_type=F32)
        for b in range(1, 4):
            summed = summed + jnp.dot(
                weights[b].astype(BF), pieces[b][:, HD:], preferred_element_type=F32
            )
        ctx[:, h * HD : (h + 1) * HD] = (summed / totals).astype(BF)

    o1.step(4)
    o1.last()
    o1.wait()
    o2.wait()

    to_d = at_tp(wrap_x(x + d), zl)
    to_minus_d = at_tp(wrap_x(x - d), zl)
    x_order = [2, d, -d, 0]
    R2 = TOK - R1

    def partial_sum(j, side):
        t = wrap_x(x + x_order[j]) * 2 + (1 - zl if side == 0 else zl)
        part[j, side] = lax.dot_general(
            ctx[...], weight_of(wo, t), (((1,), (1,)), ((), ())), preferred_element_type=F32
        ).astype(BF)

    z1, relay2, direct2, sum2 = {}, {}, {}, {}
    for j in range(4):
        for side in range(2):
            partial_sum(j, side)
            rest = part.at[j, side, pl.ds(R1, R2)]
            if side == 0:
                z1[j] = send(part.at[j, 0, pl.ds(0, R1)], z1_r.at[j], z_other)
            if j == 0:
                relay2[side] = send(rest, x2_r.at[side, 0], to_d)
            if j == 2:
                direct2[side] = send(rest, x2_r.at[side, 1], to_minus_d)

    def rows_1(j):
        return part[j, 1, pl.ds(0, R1), :].astype(F32) + z1_r[j].astype(F32)

    def rows_2(j, side):
        return part[j, side, pl.ds(R1, R2), :].astype(F32)

    z1[0].wait_recv()
    pair_s[0] = rows_1(0).astype(BF)
    relay1 = send(pair_s.at[0], x1_r.at[0], to_d)
    for side in range(2):
        relay2[side].wait_recv()
        sum2_s[side] = (rows_2(1, side) + x2_r[side, 0].astype(F32)).astype(BF)
        sum2[side] = send(sum2_s.at[side], x2_r.at[side, 2], to_d)
    z1[1].wait_recv()
    z1[2].wait_recv()
    pair_s[2] = rows_1(2).astype(BF)
    direct1 = send(pair_s.at[2], x1_r.at[1], to_minus_d)
    relay1.wait_recv()
    pair_s[1] = (rows_1(1) + x1_r[0].astype(F32)).astype(BF)
    sum1 = send(pair_s.at[1], x1_r.at[2], to_d)

    def total_2(side):
        sum2[side].wait_recv()
        direct2[side].wait_recv()
        return rows_2(3, side) + x2_r[side, 1].astype(F32) + x2_r[side, 2].astype(F32)

    z2_s[...] = total_2(0).astype(BF)
    z2 = send(z2_s, z2_r, z_other)
    mine_2 = total_2(1)
    z1[3].wait_recv()
    direct1.wait_recv()
    sum1.wait_recv()
    out_ref[pl.ds(0, R1), :] = (
        rows_1(3) + x1_r[1].astype(F32) + x1_r[2].astype(F32)
    ).astype(BF)
    z2.wait_recv()
    out_ref[pl.ds(R1, R2), :] = (mine_2 + z2_r[...].astype(F32)).astype(BF)
    for copy in started:
        copy.wait_send()


def body(rollout_rows, live_rows, doc_lengths, block_owner, norm_gain, qkv_weight, out_weight):
    positions = jnp.arange(N_SEQ, dtype=jnp.int32)
    slots = lax.rem(positions, 2) * (N_SEQ // 2) + positions // 2
    slot_of = jnp.sum(
        jnp.where(block_owner[None, :] == positions[:, None], slots[None, :], 0), axis=1
    )
    smem = pl.BlockSpec(memory_space=pltpu.SMEM)
    vmem = pl.BlockSpec(memory_space=pltpu.VMEM)
    anyw = pl.BlockSpec(memory_space=pl.ANY)
    V = pltpu.VMEM
    return pl.pallas_call(
        kernel,
        out_shape=(
            jax.ShapeDtypeStruct((TOK, COLS), BF),
            jax.ShapeDtypeStruct((TOK, HD), BF),
            jax.ShapeDtypeStruct((TOK, HD), BF),
        ),
        in_specs=[smem, smem, smem, vmem, anyw, anyw, anyw],
        out_specs=(vmem, vmem, vmem),
        scratch_shapes=[
            V((CAP, COLS), BF),
            V((2, N_Y, N_Z, BLK, 2 * HD), BF),
            V((2, N_Y, N_Z, BLK, QW), BF),
            V((2, N_Y, N_Z, BLK, QW), BF),
            V((N_TP, TOK, COLS), BF),
            V((HALF, COLS), BF),
            V((HALF, COLS), BF),
            V((8, 128), jnp.int32),
            V((8, 128), jnp.int32),
            V((N_Z, 8, 128), jnp.int32),
            V((N_Y, 8, 128), jnp.int32),
            V((N_TP, 2, 8, 128), F32),
            V((TOK, 2 * HD), F32),
            V((TOK, QW), F32),
            V((TOK, 2 * HD), BF),
            V((3, TOK, 2 * HD), BF),
            V((4, TOK, TOK), F32),
            V((TOK, QW), BF),
            V((4, 2, TOK, COLS), BF),
            V((4, R1, COLS), BF),
            V((3, R1, COLS), BF),
            V((3, R1, COLS), BF),
            V((2, 3, TOK - R1, COLS), BF),
            V((2, TOK - R1, COLS), BF),
            V((TOK - R1, COLS), BF),
            V((TOK - R1, COLS), BF),
            pltpu.SemaphoreType.DMA((4,)),
            pltpu.SemaphoreType.DMA((N_COPIES,)),
            pltpu.SemaphoreType.DMA((N_COPIES,)),
        ],
        compiler_params=pltpu.CompilerParams(collective_id=0, has_side_effects=True),
    )(
        live_rows, doc_lengths, slot_of, norm_gain.reshape(D // 128, 128),
        rollout_rows, qkv_weight, out_weight,
    )


def solution(mesh):
    in_specs = (P("seq", "tp"), P("seq"), P(), P(), P(), P("seq", "tp"), P("seq", "tp"))
    out_specs = (P("seq", "tp"), P("seq", "tp"), P("seq", "tp"))
    return jax.shard_map(body, mesh=mesh, in_specs=in_specs, out_specs=out_specs, check_vma=False)
```

```python
import jax
import jax.numpy as jnp
from jax import lax
from jax.experimental import pallas as pl
from jax.experimental.pallas import tpu as pltpu
from jax.sharding import PartitionSpec as P

D = 5120
HD = 128
GROUP = 3
TOK = 256
HALF = 128
CAP = 384
BLK = 80
N_SEQ = 64
N_TP = 8
N_Y, N_Z, N_X = 8, 4, 4
COLS = 640
QW = GROUP * HD
EPSILON = 1e-06
NEG = -1e30
N_COPIES = 200
O_FIRST = 64
R1 = 112
MESH = pl.DeviceIdType.MESH
BF = jnp.bfloat16
F32 = jnp.float32


def kernel(
    live_s, docs_s, slot_s, gain_v, roll_h, wqkv_h, wo_h,
    out_ref, key_ref, value_ref,
    rows, wkv, wq, wo, acts, tail_s, tail_r, live_y, live_c, ssq,
    acc_kv, acc_q, kv_own, kv_in, bias, ctx, part,
    z1_r, pair_s, x1_r, x2_r, sum2_s, z2_s, z2_r,
    local_sem, send_sem, recv_sem,
):
    seq = lax.axis_index("seq")
    tp = lax.axis_index("tp")
    core = lax.rem(seq, 2)
    zh = lax.rem(lax.div(seq, 2), N_Z)
    y = lax.div(seq, 2 * N_Z)
    zl = lax.rem(tp, 2)
    x = lax.div(tp, 2)
    d = 1 - 2 * core

    def wrap_y(v):
        return lax.rem(v + 2 * N_Y, N_Y)

    def wrap_z(v):
        return lax.rem(v + 2 * N_Z, N_Z)

    def wrap_x(v):
        return lax.rem(v + 2 * N_X, N_X)

    def at_seq(y_, z_, c_):
        return ((y_ * N_Z + z_) * 2 + c_, tp)

    def at_tp(x_, zl_):
        return (seq, x_ * 2 + zl_)

    partner = at_seq(y, zh, 1 - core)
    next_1 = (lax.rem(seq + 1, N_SEQ), tp)
    next_2 = (lax.rem(seq + 2, N_SEQ), tp)
    prev_1 = (lax.rem(seq + N_SEQ - 1, N_SEQ), tp)
    prev_2 = (lax.rem(seq + N_SEQ - 2, N_SEQ), tp)

    started = []

    def send(src, dst, device):
        n = len(started)
        copy = pltpu.make_async_remote_copy(
            src_ref=src, dst_ref=dst, send_sem=send_sem.at[n], recv_sem=recv_sem.at[n],
            device_id=device, device_id_type=MESH,
        )
        copy.start()
        started.append(copy)
        return copy

    loads = [
        pltpu.make_async_copy(wqkv_h.at[:, pl.ds(QW, 2 * HD)], wkv.at[core, y, zh], local_sem.at[0]),
        pltpu.make_async_copy(wqkv_h.at[:, pl.ds(0, QW)], wq.at[core, y, zh], local_sem.at[1]),
        pltpu.make_async_copy(roll_h, rows, local_sem.at[2]),
        pltpu.make_async_copy(wo_h, wo.at[core, y, zh], local_sem.at[3]),
    ]
    for load in loads:
        load.start()

    barrier = pltpu.get_barrier_semaphore()
    greeted = [partner, next_1, next_2, prev_1, prev_2]
    greeted += [at_seq(y, wrap_z(zh + k), c) for k in range(1, N_Z) for c in (core, 1 - core)]
    greeted += [at_seq(wrap_y(y + k), zh, core) for k in range(1, N_Y)]
    greeted += [(seq, lax.rem(tp + k, N_TP)) for k in range(1, N_TP)]
    for device in greeted:
        pl.semaphore_signal(barrier, inc=1, device_id=device, device_id_type=MESH)
    live_y[0] = jnp.full((8, 128), live_s[0], jnp.int32)
    gain_all = gain_v[...].astype(F32)
    gain_row = lax.broadcasted_iota(jnp.int32, (D // 128, 128), 0)
    gain = jnp.concatenate(
        [
            jnp.sum(jnp.where(gain_row == tp * 5 + i, gain_all, 0.0), axis=0, keepdims=True)
            for i in range(5)
        ],
        axis=1,
    )
    for load in loads:
        load.wait()
    own_a = rows[pl.ds(0, HALF), :].astype(F32)
    acts[tp, pl.ds(0, HALF), :] = (own_a * gain).astype(BF)
    row = lax.broadcasted_iota(jnp.int32, (HALF, CAP), 0)
    col = lax.broadcasted_iota(jnp.int32, (HALF, CAP), 1)
    chosen = (col == row + (live_s[0] - HALF)).astype(BF)
    tail_s[...] = jnp.dot(chosen, rows[...], preferred_element_type=F32).astype(BF)
    pl.semaphore_wait(barrier, len(greeted))

    up_z = at_seq(y, wrap_z(zh + d), core)
    down_z = at_seq(y, wrap_z(zh - d), core)
    up_y = at_seq(wrap_y(y + d), zh, core)
    down_y = at_seq(wrap_y(y - d), zh, core)
    z_blocks = [zh, wrap_z(zh - d), wrap_z(zh + d), wrap_z(zh + 2 * d)]

    class Gather:
        def __init__(self, buf, first, count):
            self.buf, self.first, self.count = buf, first, count
            self.up, self.down, self.across = {}, {}, []

        def block(self, y_, z_):
            whole = self.count == BLK
            return self.buf.at[core, y_, z_] if whole else (
                self.buf.at[core, y_, z_, pl.ds(self.first, self.count)])

        def line_y(self, y_):
            whole = self.count == BLK
            return self.buf.at[core, y_] if whole else (
                self.buf.at[core, y_, :, pl.ds(self.first, self.count)])

        def line_z(self, z_):
            return self.buf.at[core, :, z_, pl.ds(self.first, self.count)]

        def z_own(self):
            own = self.block(y, zh)
            self.z1, self.z2 = send(own, own, up_z), send(own, own, down_z)

        def ring(self, b, k):
            if k > 1:
                self.up[b, k - 1].wait_recv()
            elif b == 1:
                self.z1.wait_recv()
                held = self.block(y, z_blocks[1])
                self.z3 = send(held, held, up_z)
            elif b == 2:
                self.z2.wait_recv()
            elif b == 3:
                self.z3.wait_recv()
            held = self.block(wrap_y(y - (k - 1) * d), z_blocks[b])
            self.up[b, k] = send(held, held, up_y)
            if k > 1:
                self.down[b, k - 1].wait_recv()
            if k < 4:
                held = self.block(wrap_y(y + (k - 1) * d), z_blocks[b])
                self.down[b, k] = send(held, held, down_y)

        def line_across(self, y_):
            held = self.line_y(wrap_y(y_))
            self.across.append(send(held, held, partner))

        def wave(self, w):
            for b, later in enumerate((0, 1, 1, 2)):
                if 1 <= w - later <= 4:
                    self.ring(b, w - later)
            if w == 3:
                self.line_across(y)
            elif w > 3:
                self.line_across(y - (w - 3) * d)
                self.line_across(y + (w - 3) * d)

        def last(self):
            for b in range(4):
                self.up[b, 4].wait_recv()
            self.line_across(y + 4)

        def column_own(self):
            own = self.line_z(zh)
            self.c1, self.c2 = send(own, own, up_z), send(own, own, down_z)
            self.across.append(send(own, own, partner))

        def column_on(self):
            self.c1.wait_recv()
            held = self.line_z(z_blocks[1])
            self.c3 = send(held, held, up_z)
            self.across.append(send(held, held, partner))

        def column_last(self):
            self.c2.wait_recv()
            held = self.line_z(z_blocks[2])
            self.across.append(send(held, held, partner))
            self.c3.wait_recv()
            held = self.line_z(z_blocks[3])
            self.across.append(send(held, held, partner))

        def wait(self):
            for copy in self.across:
                copy.wait_recv()

    kv = Gather(wkv, 0, BLK)
    qq = Gather(wq, 0, BLK)
    o1 = Gather(wo, 0, O_FIRST)
    o2 = Gather(wo, O_FIRST, BLK - O_FIRST)

    def squares(values):
        total = jnp.sum(values * values, axis=1, keepdims=True)
        return jnp.transpose(jnp.broadcast_to(total, (HALF, 128)))[:8]

    x_up = at_tp(wrap_x(x + 1), zl)
    x_down = at_tp(wrap_x(x - 1), zl)
    z_other = at_tp(x, 1 - zl)

    class Tokens:
        def __init__(self, part):
            self.part = part

        def chunk(self, x_, zl_):
            return acts.at[wrap_x(x_) * 2 + zl_, pl.ds(self.part * HALF, HALF)]

        def own(self):
            own = self.chunk(x, zl)
            self.a = [send(own, own, z_other), send(own, own, x_up), send(own, own, x_down)]

        def second(self):
            self.a[0].wait_recv()
            held = self.chunk(x, 1 - zl)
            self.b = [send(held, held, x_up), send(held, held, x_down)]

        def third(self):
            self.a[1].wait_recv()
            held = self.chunk(x - 1, zl)
            self.c = [send(held, held, x_up)]
            self.b[1].wait_recv()
            held = self.chunk(x + 1, 1 - zl)
            self.c.append(send(held, held, x_down))

        def wait(self):
            for copy in [self.a[2], self.b[0], *self.c]:
                copy.wait_recv()

    tok_a, tok_b = Tokens(0), Tokens(1)

    live_over_y = [
        send(live_y.at[0], live_y.at[k], at_seq(wrap_y(y + k), zh, core)) for k in range(1, N_Y)
    ]
    kv.z_own()
    kv.wave(1)
    qq.z_own()
    qq.wave(1)
    tok_a.own()
    o2.ring(0, 1)
    tail = send(tail_s, tail_r, next_1)
    ssq[tp, 0] = squares(own_a)
    kv.wave(2)
    for copy in live_over_y:
        copy.wait_recv()
    earlier = jnp.zeros((8, 128), jnp.int32)
    for k in range(1, N_Y):
        earlier = earlier + live_y[k] * (k <= y).astype(jnp.int32)
    live_c[0, 0] = earlier
    live_c[0, 1] = live_y[0]
    live_over_z = [
        send(
            live_c.at[0], live_c.at[n],
            at_seq(y, wrap_z(zh + n // 2), 1 - core if n % 2 else core),
        )
        for n in range(1, 2 * N_Z)
    ]
    o2.ring(0, 2)
    qq.wave(2)
    tok_a.second()
    kv.wave(3)
    o2.ring(0, 3)
    qq.wave(3)
    tok_a.third()
    o1.z_own()

    for copy in live_over_z:
        copy.wait_recv()
    before = live_c[0, 0] - seq * TOK
    for n in range(1, 2 * N_Z):
        counts = core if n == 1 else (n // 2 <= zh).astype(jnp.int32)
        before = before + live_c[n, 0] + live_c[n, 1] * counts
    spilled = before[:1, :]
    tail.wait_recv()
    row_b = lax.broadcasted_iota(jnp.int32, (HALF, 128), 0)
    keep = jnp.broadcast_to((row_b + spilled < HALF)[:, :1], (HALF, COLS))
    own_b = jnp.where(
        keep, rows[pl.ds(HALF, HALF), :].astype(F32), tail_r[...].astype(F32)
    )
    acts[tp, pl.ds(HALF, HALF), :] = (own_b * gain).astype(BF)
    tok_b.own()
    ssq[tp, 1] = squares(own_b)
    ssq_copies = [
        send(ssq.at[tp], ssq.at[tp], (seq, lax.rem(tp + k, N_TP))) for k in range(1, N_TP)
    ]
    kv.wave(4)
    o2.ring(0, 4)
    qq.wave(4)
    tok_b.second()
    o2.up[0, 4].wait_recv()
    o2.column_own()
    kv.wave(5)

    position = seq * TOK + lax.broadcasted_iota(jnp.int32, (TOK, 128), 0)
    first = jnp.zeros((TOK, 128), jnp.int32)
    begin = docs_s[0]
    for doc in range(1, 32):
        first = jnp.maximum(first, jnp.where(position >= begin, begin, 0))
        begin = begin + docs_s[doc]
    key_base = [seq, seq - 2, seq - 3 + 2 * core, seq - 1 - 2 * core]
    lane = lax.broadcasted_iota(jnp.int32, (TOK, 128), 1)
    for b in range(4):
        for side in range(2):
            key_pos = key_base[b] * TOK + side * 128 + lane
            allowed = (key_pos <= position) & (key_pos >= first)
            bias[b, :, pl.ds(side * 128, 128)] = jnp.where(allowed, 0.0, NEG)

    qq.wave(5)
    tok_b.third()
    o1.wave(1)
    o2.column_on()
    kv.wave(6)
    kv.last()
    qq.wave(6)
    o1.wave(2)
    o1.wave(3)

    def weight_of(buf, t):
        blocks = []
        for i in range(8):
            s = slot_s[t * 8 + i]
            blocks.append(
                buf[lax.div(s, N_Y * N_Z), lax.rem(lax.div(s, N_Z), N_Y), lax.rem(s, N_Z)]
            )
        return jnp.concatenate(blocks, axis=0)

    def project(buf, total):
        total[...] = jnp.zeros_like(total)

        def one(t, carry):
            total[...] += jnp.dot(acts[t], weight_of(buf, t), preferred_element_type=F32)
            return carry

        lax.fori_loop(0, N_TP, one, 0)

    tok_a.wait()
    tok_b.wait()
    for copy in ssq_copies:
        copy.wait_recv()
    kv.wait()
    project(wkv, acc_kv)

    total = ssq[0]
    for t in range(1, N_TP):
        total = total + ssq[t]
    scale_row = lax.rsqrt(total * (1.0 / D) + EPSILON)
    scale = jnp.concatenate(
        [jnp.transpose(jnp.broadcast_to(scale_row[h, :1], (128, 128))) for h in range(2)], axis=0
    )
    turn_row = lax.broadcasted_iota(jnp.int32, (TOK, TOK), 0)
    turn_col = lax.broadcasted_iota(jnp.int32, (TOK, TOK), 1)
    spilled_wide = jnp.concatenate([spilled, spilled], axis=1)
    turn = (((turn_col - turn_row + spilled_wide + TOK) & (TOK - 1)) == 0).astype(BF)

    def in_order(values):
        return jnp.dot(turn, values, preferred_element_type=F32).astype(BF)

    keys = in_order((acc_kv[:, :HD] * scale).astype(BF))
    values = in_order((acc_kv[:, HD:] * scale).astype(BF))
    kv_own[:, :HD] = keys
    kv_own[:, HD:] = values
    kv_1 = send(kv_own, kv_in.at[0], next_2)
    n_kv = len(started)

    def kv_copy(src):
        return pltpu.make_async_remote_copy(
            src_ref=src, dst_ref=kv_in.at[1], send_sem=send_sem.at[n_kv],
            recv_sem=recv_sem.at[n_kv], device_id=next_1, device_id_type=MESH,
        )

    @pl.when(core == 0)
    def _():
        kv_copy(kv_own).start()

    kv_2 = kv_copy(kv_own)
    started.append(kv_2)
    key_ref[...] = keys
    value_ref[...] = values
    qq.last()
    o1.wave(4)
    qq.wait()
    project(wq, acc_q)
    queries = [
        in_order((acc_q[:, h * HD : (h + 1) * HD] * scale * HD ** (-0.5)).astype(BF))
        for h in range(GROUP)
    ]
    kv_1.wait_recv()

    @pl.when(core == 1)
    def _():
        kv_copy(kv_in.at[0]).start()

    kv_3 = send(kv_in.at[0], kv_in.at[2], partner)
    o1.wave(5)
    o2.column_last()
    o1.wave(6)
    kv_2.wait_recv()
    kv_3.wait_recv()

    pieces = [kv_own, kv_in.at[0], kv_in.at[1], kv_in.at[2]]
    for h in range(GROUP):
        scores = [
            lax.dot_general(
                queries[h], pieces[b][:, :HD], (((1,), (1,)), ((), ())),
                preferred_element_type=F32,
            ) + bias[b]
            for b in range(4)
        ]
        best = jnp.maximum(
            jnp.maximum(scores[0], scores[1]), jnp.maximum(scores[2], scores[3])
        )
        best = jnp.max(best, axis=1, keepdims=True)
        weights = [jnp.exp(s - best) for s in scores]
        totals = jnp.sum(weights[0] + weights[1] + weights[2] + weights[3], axis=1, keepdims=True)
        summed = jnp.dot(weights[0].astype(BF), pieces[0][:, HD:], preferred_element_type=F32)
        for b in range(1, 4):
            summed = summed + jnp.dot(
                weights[b].astype(BF), pieces[b][:, HD:], preferred_element_type=F32
            )
        ctx[:, h * HD : (h + 1) * HD] = (summed / totals).astype(BF)

    o1.last()
    o1.wait()
    o2.wait()

    to_d = at_tp(wrap_x(x + d), zl)
    to_minus_d = at_tp(wrap_x(x - d), zl)
    x_order = [2, d, -d, 0]
    R2 = TOK - R1

    def partial_sum(j, side):
        t = wrap_x(x + x_order[j]) * 2 + (1 - zl if side == 0 else zl)
        part[j, side] = lax.dot_general(
            ctx[...], weight_of(wo, t), (((1,), (1,)), ((), ())), preferred_element_type=F32
        ).astype(BF)

    z1, relay2, direct2, sum2 = {}, {}, {}, {}
    for j in range(4):
        for side in range(2):
            partial_sum(j, side)
            rest = part.at[j, side, pl.ds(R1, R2)]
            if side == 0:
                z1[j] = send(part.at[j, 0, pl.ds(0, R1)], z1_r.at[j], z_other)
            if j == 0:
                relay2[side] = send(rest, x2_r.at[side, 0], to_d)
            if j == 2:
                direct2[side] = send(rest, x2_r.at[side, 1], to_minus_d)

    def rows_1(j):
        return part[j, 1, pl.ds(0, R1), :].astype(F32) + z1_r[j].astype(F32)

    def rows_2(j, side):
        return part[j, side, pl.ds(R1, R2), :].astype(F32)

    z1[0].wait_recv()
    pair_s[0] = rows_1(0).astype(BF)
    relay1 = send(pair_s.at[0], x1_r.at[0], to_d)
    for side in range(2):
        relay2[side].wait_recv()
        sum2_s[side] = (rows_2(1, side) + x2_r[side, 0].astype(F32)).astype(BF)
        sum2[side] = send(sum2_s.at[side], x2_r.at[side, 2], to_d)
    z1[1].wait_recv()
    z1[2].wait_recv()
    pair_s[2] = rows_1(2).astype(BF)
    direct1 = send(pair_s.at[2], x1_r.at[1], to_minus_d)
    relay1.wait_recv()
    pair_s[1] = (rows_1(1) + x1_r[0].astype(F32)).astype(BF)
    sum1 = send(pair_s.at[1], x1_r.at[2], to_d)

    def total_2(side):
        sum2[side].wait_recv()
        direct2[side].wait_recv()
        return rows_2(3, side) + x2_r[side, 1].astype(F32) + x2_r[side, 2].astype(F32)

    z2_s[...] = total_2(0).astype(BF)
    z2 = send(z2_s, z2_r, z_other)
    mine_2 = total_2(1)
    z1[3].wait_recv()
    direct1.wait_recv()
    sum1.wait_recv()
    out_ref[pl.ds(0, R1), :] = (
        rows_1(3) + x1_r[1].astype(F32) + x1_r[2].astype(F32)
    ).astype(BF)
    z2.wait_recv()
    out_ref[pl.ds(R1, R2), :] = (mine_2 + z2_r[...].astype(F32)).astype(BF)
    for copy in started:
        copy.wait_send()


def body(rollout_rows, live_rows, doc_lengths, block_owner, norm_gain, qkv_weight, out_weight):
    positions = jnp.arange(N_SEQ, dtype=jnp.int32)
    slots = lax.rem(positions, 2) * (N_SEQ // 2) + positions // 2
    slot_of = jnp.sum(
        jnp.where(block_owner[None, :] == positions[:, None], slots[None, :], 0), axis=1
    )
    smem = pl.BlockSpec(memory_space=pltpu.SMEM)
    vmem = pl.BlockSpec(memory_space=pltpu.VMEM)
    anyw = pl.BlockSpec(memory_space=pl.ANY)
    V = pltpu.VMEM
    return pl.pallas_call(
        kernel,
        out_shape=(
            jax.ShapeDtypeStruct((TOK, COLS), BF),
            jax.ShapeDtypeStruct((TOK, HD), BF),
            jax.ShapeDtypeStruct((TOK, HD), BF),
        ),
        in_specs=[smem, smem, smem, vmem, anyw, anyw, anyw],
        out_specs=(vmem, vmem, vmem),
        scratch_shapes=[
            V((CAP, COLS), BF),
            V((2, N_Y, N_Z, BLK, 2 * HD), BF),
            V((2, N_Y, N_Z, BLK, QW), BF),
            V((2, N_Y, N_Z, BLK, QW), BF),
            V((N_TP, TOK, COLS), BF),
            V((HALF, COLS), BF),
            V((HALF, COLS), BF),
            V((N_Y, 8, 128), jnp.int32),
            V((2 * N_Z, 2, 8, 128), jnp.int32),
            V((N_TP, 2, 8, 128), F32),
            V((TOK, 2 * HD), F32),
            V((TOK, QW), F32),
            V((TOK, 2 * HD), BF),
            V((3, TOK, 2 * HD), BF),
            V((4, TOK, TOK), F32),
            V((TOK, QW), BF),
            V((4, 2, TOK, COLS), BF),
            V((4, R1, COLS), BF),
            V((3, R1, COLS), BF),
            V((3, R1, COLS), BF),
            V((2, 3, TOK - R1, COLS), BF),
            V((2, TOK - R1, COLS), BF),
            V((TOK - R1, COLS), BF),
            V((TOK - R1, COLS), BF),
            pltpu.SemaphoreType.DMA((4,)),
            pltpu.SemaphoreType.DMA((N_COPIES,)),
            pltpu.SemaphoreType.DMA((N_COPIES,)),
        ],
        compiler_params=pltpu.CompilerParams(collective_id=0, has_side_effects=True),
    )(
        live_rows, doc_lengths, slot_of, norm_gain.reshape(D // 128, 128),
        rollout_rows, qkv_weight, out_weight,
    )


def solution(mesh):
    in_specs = (P("seq", "tp"), P("seq"), P(), P(), P(), P("seq", "tp"), P("seq", "tp"))
    out_specs = (P("seq", "tp"), P("seq", "tp"), P("seq", "tp"))
    return jax.shard_map(body, mesh=mesh, in_specs=in_specs, out_specs=out_specs, check_vma=False)
```

```python
import jax
import jax.numpy as jnp
from jax import lax
from jax.experimental import pallas as pl
from jax.experimental.pallas import tpu as pltpu
from jax.sharding import PartitionSpec as P

D = 5120
HD = 128
GROUP = 3
TOK = 256
HALF = 128
CAP = 384
BLK = 80
N_SEQ = 64
N_TP = 8
N_Y, N_Z, N_X = 8, 4, 4
COLS = 640
QW = GROUP * HD
EPSILON = 1e-06
NEG = -1e30
N_COPIES = 200
O_FIRST = 64
R1 = 112
MESH = pl.DeviceIdType.MESH
BF = jnp.bfloat16
F32 = jnp.float32


def kernel(
    live_s, docs_s, owner_s, gain_v, roll_h, wqkv_h, wo_h,
    out_ref, key_ref, value_ref,
    rows, wkv, wq, wo, acts, tail_s, tail_r, live_y, live_c, ssq,
    slot_v, slot_s, acc_kv, acc_q, kv_own, kv_in, bias, ctx, part,
    z1_r, pair_s, x1_r, x2_r, sum2_s, z2_s, z2_r,
    local_sem, send_sem, recv_sem,
):
    seq = lax.axis_index("seq")
    tp = lax.axis_index("tp")
    core = lax.rem(seq, 2)
    zh = lax.rem(lax.div(seq, 2), N_Z)
    y = lax.div(seq, 2 * N_Z)
    zl = lax.rem(tp, 2)
    x = lax.div(tp, 2)
    d = 1 - 2 * core

    def wrap_y(v):
        return lax.rem(v + 2 * N_Y, N_Y)

    def wrap_z(v):
        return lax.rem(v + 2 * N_Z, N_Z)

    def wrap_x(v):
        return lax.rem(v + 2 * N_X, N_X)

    def at_seq(y_, z_, c_):
        return ((y_ * N_Z + z_) * 2 + c_, tp)

    def at_tp(x_, zl_):
        return (seq, x_ * 2 + zl_)

    partner = at_seq(y, zh, 1 - core)
    next_1 = (lax.rem(seq + 1, N_SEQ), tp)
    next_2 = (lax.rem(seq + 2, N_SEQ), tp)
    prev_1 = (lax.rem(seq + N_SEQ - 1, N_SEQ), tp)
    prev_2 = (lax.rem(seq + N_SEQ - 2, N_SEQ), tp)

    started = []

    def send(src, dst, device):
        n = len(started)
        copy = pltpu.make_async_remote_copy(
            src_ref=src, dst_ref=dst, send_sem=send_sem.at[n], recv_sem=recv_sem.at[n],
            device_id=device, device_id_type=MESH,
        )
        copy.start()
        started.append(copy)
        return copy

    loads = [
        pltpu.make_async_copy(wqkv_h.at[:, pl.ds(QW, 2 * HD)], wkv.at[core, y, zh], local_sem.at[0]),
        pltpu.make_async_copy(wqkv_h.at[:, pl.ds(0, QW)], wq.at[core, y, zh], local_sem.at[1]),
        pltpu.make_async_copy(roll_h, rows, local_sem.at[2]),
        pltpu.make_async_copy(wo_h, wo.at[core, y, zh], local_sem.at[3]),
    ]
    for load in loads:
        load.start()

    barrier = pltpu.get_barrier_semaphore()
    greeted = [partner, next_1, next_2, prev_1, prev_2]
    greeted += [at_seq(y, wrap_z(zh + k), c) for k in range(1, N_Z) for c in (core, 1 - core)]
    greeted += [at_seq(wrap_y(y + k), zh, core) for k in range(1, N_Y)]
    greeted += [(seq, lax.rem(tp + k, N_TP)) for k in range(1, N_TP)]
    for device in greeted:
        pl.semaphore_signal(barrier, inc=1, device_id=device, device_id_type=MESH)
    live_y[0] = jnp.full((8, 128), live_s[0], jnp.int32)
    block = lax.broadcasted_iota(jnp.int32, (8, 128), 1)
    place = jnp.zeros((8, 128), jnp.int32)
    for j in range(N_SEQ):
        place = jnp.where(block == owner_s[j], (j % 2) * (N_SEQ // 2) + j // 2, place)
    slot_v[...] = place
    gain_all = gain_v[...].astype(F32)
    gain_row = lax.broadcasted_iota(jnp.int32, (D // 128, 128), 0)
    gain = jnp.concatenate(
        [
            jnp.sum(jnp.where(gain_row == tp * 5 + i, gain_all, 0.0), axis=0, keepdims=True)
            for i in range(5)
        ],
        axis=1,
    )
    for load in loads:
        load.wait()
    own_a = rows[pl.ds(0, HALF), :].astype(F32)
    acts[tp, pl.ds(0, HALF), :] = (own_a * gain).astype(BF)
    row = lax.broadcasted_iota(jnp.int32, (HALF, CAP), 0)
    col = lax.broadcasted_iota(jnp.int32, (HALF, CAP), 1)
    chosen = (col == row + (live_s[0] - HALF)).astype(BF)
    tail_s[...] = jnp.dot(chosen, rows[...], preferred_element_type=F32).astype(BF)
    slots = pltpu.make_async_copy(slot_v, slot_s, local_sem.at[4])
    slots.start()
    pl.semaphore_wait(barrier, len(greeted))

    up_z = at_seq(y, wrap_z(zh + d), core)
    down_z = at_seq(y, wrap_z(zh - d), core)
    up_y = at_seq(wrap_y(y + d), zh, core)
    down_y = at_seq(wrap_y(y - d), zh, core)
    z_blocks = [zh, wrap_z(zh - d), wrap_z(zh + d), wrap_z(zh + 2 * d)]

    class Gather:
        def __init__(self, buf, first, count):
            self.buf, self.first, self.count = buf, first, count
            self.up, self.down, self.across = {}, {}, []

        def block(self, y_, z_):
            whole = self.count == BLK
            return self.buf.at[core, y_, z_] if whole else (
                self.buf.at[core, y_, z_, pl.ds(self.first, self.count)])

        def line_y(self, y_):
            whole = self.count == BLK
            return self.buf.at[core, y_] if whole else (
                self.buf.at[core, y_, :, pl.ds(self.first, self.count)])

        def line_z(self, z_):
            return self.buf.at[core, :, z_, pl.ds(self.first, self.count)]

        def z_own(self):
            own = self.block(y, zh)
            self.z1, self.z2 = send(own, own, up_z), send(own, own, down_z)

        def ring(self, b, k):
            if k > 1:
                self.up[b, k - 1].wait_recv()
            elif b == 1:
                self.z1.wait_recv()
                held = self.block(y, z_blocks[1])
                self.z3 = send(held, held, up_z)
            elif b == 2:
                self.z2.wait_recv()
            elif b == 3:
                self.z3.wait_recv()
            held = self.block(wrap_y(y - (k - 1) * d), z_blocks[b])
            self.up[b, k] = send(held, held, up_y)
            if k > 1:
                self.down[b, k - 1].wait_recv()
            if k < 4:
                held = self.block(wrap_y(y + (k - 1) * d), z_blocks[b])
                self.down[b, k] = send(held, held, down_y)

        def line_across(self, y_):
            held = self.line_y(wrap_y(y_))
            self.across.append(send(held, held, partner))

        def wave(self, w):
            for b, later in enumerate((0, 1, 1, 2)):
                if 1 <= w - later <= 4:
                    self.ring(b, w - later)
            if w == 3:
                self.line_across(y)
            elif w > 3:
                self.line_across(y - (w - 3) * d)
                self.line_across(y + (w - 3) * d)

        def last(self):
            for b in range(4):
                self.up[b, 4].wait_recv()
            self.line_across(y + 4)

        def column_own(self):
            own = self.line_z(zh)
            self.c1, self.c2 = send(own, own, up_z), send(own, own, down_z)
            self.across.append(send(own, own, partner))

        def column_on(self):
            self.c1.wait_recv()
            held = self.line_z(z_blocks[1])
            self.c3 = send(held, held, up_z)
            self.across.append(send(held, held, partner))

        def column_last(self):
            self.c2.wait_recv()
            held = self.line_z(z_blocks[2])
            self.across.append(send(held, held, partner))
            self.c3.wait_recv()
            held = self.line_z(z_blocks[3])
            self.across.append(send(held, held, partner))

        def wait(self):
            for copy in self.across:
                copy.wait_recv()

    kv = Gather(wkv, 0, BLK)
    qq = Gather(wq, 0, BLK)
    o1 = Gather(wo, 0, O_FIRST)
    o2 = Gather(wo, O_FIRST, BLK - O_FIRST)

    def squares(values):
        total = jnp.sum(values * values, axis=1, keepdims=True)
        return jnp.transpose(jnp.broadcast_to(total, (HALF, 128)))[:8]

    x_up = at_tp(wrap_x(x + 1), zl)
    x_down = at_tp(wrap_x(x - 1), zl)
    z_other = at_tp(x, 1 - zl)

    class Tokens:
        def __init__(self, part):
            self.part = part

        def chunk(self, x_, zl_):
            return acts.at[wrap_x(x_) * 2 + zl_, pl.ds(self.part * HALF, HALF)]

        def own(self):
            own = self.chunk(x, zl)
            self.a = [send(own, own, z_other), send(own, own, x_up), send(own, own, x_down)]

        def second(self):
            self.a[0].wait_recv()
            held = self.chunk(x, 1 - zl)
            self.b = [send(held, held, x_up), send(held, held, x_down)]

        def third(self):
            self.a[1].wait_recv()
            held = self.chunk(x - 1, zl)
            self.c = [send(held, held, x_up)]
            self.b[1].wait_recv()
            held = self.chunk(x + 1, 1 - zl)
            self.c.append(send(held, held, x_down))

        def wait(self):
            for copy in [self.a[2], self.b[0], *self.c]:
                copy.wait_recv()

    tok_a, tok_b = Tokens(0), Tokens(1)

    live_over_y = [
        send(live_y.at[0], live_y.at[k], at_seq(wrap_y(y + k), zh, core)) for k in range(1, N_Y)
    ]
    kv.z_own()
    kv.wave(1)
    qq.z_own()
    qq.wave(1)
    tok_a.own()
    o2.ring(0, 1)
    tail = send(tail_s, tail_r, next_1)
    ssq[tp, 0] = squares(own_a)
    kv.wave(2)
    for copy in live_over_y:
        copy.wait_recv()
    earlier = jnp.zeros((8, 128), jnp.int32)
    for k in range(1, N_Y):
        earlier = earlier + live_y[k] * (k <= y).astype(jnp.int32)
    live_c[0, 0] = earlier
    live_c[0, 1] = live_y[0]
    live_over_z = [
        send(
            live_c.at[0], live_c.at[n],
            at_seq(y, wrap_z(zh + n // 2), 1 - core if n % 2 else core),
        )
        for n in range(1, 2 * N_Z)
    ]
    o2.ring(0, 2)
    qq.wave(2)
    tok_a.second()
    kv.wave(3)
    o2.ring(0, 3)
    qq.wave(3)
    tok_a.third()
    o1.z_own()

    for copy in live_over_z:
        copy.wait_recv()
    before = live_c[0, 0] - seq * TOK
    for n in range(1, 2 * N_Z):
        counts = core if n == 1 else (n // 2 <= zh).astype(jnp.int32)
        before = before + live_c[n, 0] + live_c[n, 1] * counts
    spilled = before[:1, :]
    tail.wait_recv()
    row_b = lax.broadcasted_iota(jnp.int32, (HALF, 128), 0)
    keep = jnp.broadcast_to((row_b + spilled < HALF)[:, :1], (HALF, COLS))
    own_b = jnp.where(
        keep, rows[pl.ds(HALF, HALF), :].astype(F32), tail_r[...].astype(F32)
    )
    acts[tp, pl.ds(HALF, HALF), :] = (own_b * gain).astype(BF)
    tok_b.own()
    ssq[tp, 1] = squares(own_b)
    ssq_copies = [
        send(ssq.at[tp], ssq.at[tp], (seq, lax.rem(tp + k, N_TP))) for k in range(1, N_TP)
    ]
    kv.wave(4)
    o2.ring(0, 4)
    qq.wave(4)
    tok_b.second()
    o2.up[0, 4].wait_recv()
    o2.column_own()
    kv.wave(5)

    position = seq * TOK + lax.broadcasted_iota(jnp.int32, (TOK, 128), 0)
    first = jnp.zeros((TOK, 128), jnp.int32)
    begin = docs_s[0]
    for doc in range(1, 32):
        first = jnp.maximum(first, jnp.where(position >= begin, begin, 0))
        begin = begin + docs_s[doc]
    key_base = [seq, seq - 2, seq - 3 + 2 * core, seq - 1 - 2 * core]
    lane = lax.broadcasted_iota(jnp.int32, (TOK, 128), 1)
    for b in range(4):
        for side in range(2):
            key_pos = key_base[b] * TOK + side * 128 + lane
            allowed = (key_pos <= position) & (key_pos >= first)
            bias[b, :, pl.ds(side * 128, 128)] = jnp.where(allowed, 0.0, NEG)

    qq.wave(5)
    tok_b.third()
    o1.wave(1)
    o2.column_on()
    kv.wave(6)
    qq.wave(6)
    o1.wave(2)
    kv.last()
    o1.wave(3)

    def weight_of(buf, t):
        blocks = []
        for i in range(8):
            s = slot_s[0, t * 8 + i]
            blocks.append(
                buf[lax.div(s, N_Y * N_Z), lax.rem(lax.div(s, N_Z), N_Y), lax.rem(s, N_Z)]
            )
        return jnp.concatenate(blocks, axis=0)

    def project(buf, total):
        total[...] = jnp.zeros_like(total)

        def one(t, carry):
            total[...] += jnp.dot(acts[t], weight_of(buf, t), preferred_element_type=F32)
            return carry

        lax.fori_loop(0, N_TP, one, 0)

    slots.wait()
    tok_a.wait()
    tok_b.wait()
    for copy in ssq_copies:
        copy.wait_recv()
    kv.wait()
    project(wkv, acc_kv)

    total = ssq[0]
    for t in range(1, N_TP):
        total = total + ssq[t]
    scale_row = lax.rsqrt(total * (1.0 / D) + EPSILON)
    scale = jnp.concatenate(
        [jnp.transpose(jnp.broadcast_to(scale_row[h, :1], (128, 128))) for h in range(2)], axis=0
    )
    turn_row = lax.broadcasted_iota(jnp.int32, (TOK, TOK), 0)
    turn_col = lax.broadcasted_iota(jnp.int32, (TOK, TOK), 1)
    spilled_wide = jnp.concatenate([spilled, spilled], axis=1)
    turn = (((turn_col - turn_row + spilled_wide + TOK) & (TOK - 1)) == 0).astype(BF)

    def in_order(values):
        return jnp.dot(turn, values, preferred_element_type=F32).astype(BF)

    keys = in_order((acc_kv[:, :HD] * scale).astype(BF))
    values = in_order((acc_kv[:, HD:] * scale).astype(BF))
    kv_own[:, :HD] = keys
    kv_own[:, HD:] = values
    kv_1 = send(kv_own, kv_in.at[0], next_2)
    n_kv = len(started)

    def kv_copy(src):
        return pltpu.make_async_remote_copy(
            src_ref=src, dst_ref=kv_in.at[1], send_sem=send_sem.at[n_kv],
            recv_sem=recv_sem.at[n_kv], device_id=next_1, device_id_type=MESH,
        )

    @pl.when(core == 0)
    def _():
        kv_copy(kv_own).start()

    kv_2 = kv_copy(kv_own)
    started.append(kv_2)
    key_ref[...] = keys
    value_ref[...] = values
    qq.last()
    o1.wave(4)
    qq.wait()
    project(wq, acc_q)
    queries = [
        in_order((acc_q[:, h * HD : (h + 1) * HD] * scale * HD ** (-0.5)).astype(BF))
        for h in range(GROUP)
    ]
    o1.wave(5)
    kv_1.wait_recv()

    @pl.when(core == 1)
    def _():
        kv_copy(kv_in.at[0]).start()

    kv_3 = send(kv_in.at[0], kv_in.at[2], partner)
    o1.wave(6)
    o2.column_last()
    o1.last()
    kv_2.wait_recv()
    kv_3.wait_recv()

    pieces = [kv_own, kv_in.at[0], kv_in.at[1], kv_in.at[2]]
    for h in range(GROUP):
        scores = [
            lax.dot_general(
                queries[h], pieces[b][:, :HD], (((1,), (1,)), ((), ())),
                preferred_element_type=F32,
            ) + bias[b]
            for b in range(4)
        ]
        best = jnp.maximum(
            jnp.maximum(scores[0], scores[1]), jnp.maximum(scores[2], scores[3])
        )
        best = jnp.max(best, axis=1, keepdims=True)
        weights = [jnp.exp(s - best) for s in scores]
        totals = jnp.sum(weights[0] + weights[1] + weights[2] + weights[3], axis=1, keepdims=True)
        summed = jnp.dot(weights[0].astype(BF), pieces[0][:, HD:], preferred_element_type=F32)
        for b in range(1, 4):
            summed = summed + jnp.dot(
                weights[b].astype(BF), pieces[b][:, HD:], preferred_element_type=F32
            )
        ctx[:, h * HD : (h + 1) * HD] = (summed / totals).astype(BF)

    o1.wait()
    o2.wait()

    to_d = at_tp(wrap_x(x + d), zl)
    to_minus_d = at_tp(wrap_x(x - d), zl)
    x_order = [2, d, -d, 0]
    R2 = TOK - R1

    def partial_sum(j, side):
        t = wrap_x(x + x_order[j]) * 2 + (1 - zl if side == 0 else zl)
        part[j, side] = lax.dot_general(
            ctx[...], weight_of(wo, t), (((1,), (1,)), ((), ())), preferred_element_type=F32
        ).astype(BF)

    z1, relay2, direct2, sum2 = {}, {}, {}, {}
    for j in range(4):
        for side in range(2):
            partial_sum(j, side)
            rest = part.at[j, side, pl.ds(R1, R2)]
            if side == 0:
                z1[j] = send(part.at[j, 0, pl.ds(0, R1)], z1_r.at[j], z_other)
            if j == 0:
                relay2[side] = send(rest, x2_r.at[side, 0], to_d)
            if j == 2:
                direct2[side] = send(rest, x2_r.at[side, 1], to_minus_d)

    def rows_1(j):
        return part[j, 1, pl.ds(0, R1), :].astype(F32) + z1_r[j].astype(F32)

    def rows_2(j, side):
        return part[j, side, pl.ds(R1, R2), :].astype(F32)

    z1[0].wait_recv()
    pair_s[0] = rows_1(0).astype(BF)
    relay1 = send(pair_s.at[0], x1_r.at[0], to_d)
    for side in range(2):
        relay2[side].wait_recv()
        sum2_s[side] = (rows_2(1, side) + x2_r[side, 0].astype(F32)).astype(BF)
        sum2[side] = send(sum2_s.at[side], x2_r.at[side, 2], to_d)
    z1[1].wait_recv()
    z1[2].wait_recv()
    pair_s[2] = rows_1(2).astype(BF)
    direct1 = send(pair_s.at[2], x1_r.at[1], to_minus_d)
    relay1.wait_recv()
    pair_s[1] = (rows_1(1) + x1_r[0].astype(F32)).astype(BF)
    sum1 = send(pair_s.at[1], x1_r.at[2], to_d)

    def total_2(side):
        sum2[side].wait_recv()
        direct2[side].wait_recv()
        return rows_2(3, side) + x2_r[side, 1].astype(F32) + x2_r[side, 2].astype(F32)

    z2_s[...] = total_2(0).astype(BF)
    z2 = send(z2_s, z2_r, z_other)
    mine_2 = total_2(1)
    z1[3].wait_recv()
    direct1.wait_recv()
    sum1.wait_recv()
    out_ref[pl.ds(0, R1), :] = (
        rows_1(3) + x1_r[1].astype(F32) + x1_r[2].astype(F32)
    ).astype(BF)
    z2.wait_recv()
    out_ref[pl.ds(R1, R2), :] = (mine_2 + z2_r[...].astype(F32)).astype(BF)
    for copy in started:
        copy.wait_send()


def body(rollout_rows, live_rows, doc_lengths, block_owner, norm_gain, qkv_weight, out_weight):
    smem = pl.BlockSpec(memory_space=pltpu.SMEM)
    vmem = pl.BlockSpec(memory_space=pltpu.VMEM)
    anyw = pl.BlockSpec(memory_space=pl.ANY)
    V = pltpu.VMEM
    return pl.pallas_call(
        kernel,
        out_shape=(
            pltpu.VMEM((TOK, COLS), BF),
            pltpu.VMEM((TOK, HD), BF),
            pltpu.VMEM((TOK, HD), BF),
        ),
        in_specs=[smem, smem, smem, vmem, anyw, anyw, anyw],
        out_specs=(vmem, vmem, vmem),
        scratch_shapes=[
            V((CAP, COLS), BF),
            V((2, N_Y, N_Z, BLK, 2 * HD), BF),
            V((2, N_Y, N_Z, BLK, QW), BF),
            V((2, N_Y, N_Z, BLK, QW), BF),
            V((N_TP, TOK, COLS), BF),
            V((HALF, COLS), BF),
            V((HALF, COLS), BF),
            V((N_Y, 8, 128), jnp.int32),
            V((2 * N_Z, 2, 8, 128), jnp.int32),
            V((N_TP, 2, 8, 128), F32),
            V((8, 128), jnp.int32),
            pltpu.SMEM((8, 128), jnp.int32),
            V((TOK, 2 * HD), F32),
            V((TOK, QW), F32),
            V((TOK, 2 * HD), BF),
            V((3, TOK, 2 * HD), BF),
            V((4, TOK, TOK), F32),
            V((TOK, QW), BF),
            V((4, 2, TOK, COLS), BF),
            V((4, R1, COLS), BF),
            V((3, R1, COLS), BF),
            V((3, R1, COLS), BF),
            V((2, 3, TOK - R1, COLS), BF),
            V((2, TOK - R1, COLS), BF),
            V((TOK - R1, COLS), BF),
            V((TOK - R1, COLS), BF),
            pltpu.SemaphoreType.DMA((5,)),
            pltpu.SemaphoreType.DMA((N_COPIES,)),
            pltpu.SemaphoreType.DMA((N_COPIES,)),
        ],
        compiler_params=pltpu.CompilerParams(collective_id=0, has_side_effects=True),
    )(
        live_rows, doc_lengths, block_owner, norm_gain.reshape(D // 128, 128),
        rollout_rows, qkv_weight, out_weight,
    )


def solution(mesh):
    in_specs = (P("seq", "tp"), P("seq"), P(), P(), P(), P("seq", "tp"), P("seq", "tp"))
    out_specs = (P("seq", "tp"), P("seq", "tp"), P("seq", "tp"))
    return jax.shard_map(body, mesh=mesh, in_specs=in_specs, out_specs=out_specs, check_vma=False)
```

```python
import jax
import jax.numpy as jnp
from jax import lax
from jax.experimental import pallas as pl
from jax.experimental.pallas import tpu as pltpu
from jax.sharding import PartitionSpec as P

D = 5120
HD = 128
GROUP = 3
TOK = 256
HALF = 128
CAP = 384
BLK = 80
N_SEQ = 64
N_TP = 8
N_Y, N_Z, N_X = 8, 4, 4
COLS = 640
QW = GROUP * HD
EPSILON = 1e-06
NEG = -1e30
N_COPIES = 200
O_FIRST = 64
R1 = 112
MESH = pl.DeviceIdType.MESH
BF = jnp.bfloat16
F32 = jnp.float32


def kernel(
    live_s, docs_s, owner_s, gain_v, roll_h, wqkv_h, wo_h,
    out_ref, key_ref, value_ref,
    rows, wkv, wq, wo, acts, tail_s, tail_r, live_y, live_c, ssq,
    slot_v, slot_s, acc_kv, acc_q, kv_own, kv_in, bias, ctx, part,
    z1_r, pair_s, x1_r, x2_r, sum2_s, z2_s, z2_r,
    local_sem, send_sem, recv_sem,
):
    seq = lax.axis_index("seq")
    tp = lax.axis_index("tp")
    core = lax.rem(seq, 2)
    zh = lax.rem(lax.div(seq, 2), N_Z)
    y = lax.div(seq, 2 * N_Z)
    zl = lax.rem(tp, 2)
    x = lax.div(tp, 2)
    d = 1 - 2 * core

    def wrap_y(v):
        return lax.rem(v + 2 * N_Y, N_Y)

    def wrap_z(v):
        return lax.rem(v + 2 * N_Z, N_Z)

    def wrap_x(v):
        return lax.rem(v + 2 * N_X, N_X)

    def at_seq(y_, z_, c_):
        return ((y_ * N_Z + z_) * 2 + c_, tp)

    def at_tp(x_, zl_):
        return (seq, x_ * 2 + zl_)

    partner = at_seq(y, zh, 1 - core)
    next_1 = (lax.rem(seq + 1, N_SEQ), tp)
    next_2 = (lax.rem(seq + 2, N_SEQ), tp)
    prev_1 = (lax.rem(seq + N_SEQ - 1, N_SEQ), tp)
    prev_2 = (lax.rem(seq + N_SEQ - 2, N_SEQ), tp)

    started = []

    def send(src, dst, device):
        n = len(started)
        copy = pltpu.make_async_remote_copy(
            src_ref=src, dst_ref=dst, send_sem=send_sem.at[n], recv_sem=recv_sem.at[n],
            device_id=device, device_id_type=MESH,
        )
        copy.start()
        started.append(copy)
        return copy

    loads = [
        pltpu.make_async_copy(wqkv_h.at[:, pl.ds(QW, 2 * HD)], wkv.at[core, y, zh], local_sem.at[0]),
        pltpu.make_async_copy(wqkv_h.at[:, pl.ds(0, QW)], wq.at[core, y, zh], local_sem.at[1]),
        pltpu.make_async_copy(roll_h, rows, local_sem.at[2]),
        pltpu.make_async_copy(wo_h, wo.at[core, y, zh], local_sem.at[3]),
    ]
    for load in loads:
        load.start()

    barrier = pltpu.get_barrier_semaphore()
    greeted = [partner, next_1, next_2, prev_1, prev_2]
    greeted += [at_seq(y, wrap_z(zh + k), c) for k in range(1, N_Z) for c in (core, 1 - core)]
    greeted += [at_seq(wrap_y(y + k), zh, core) for k in range(1, N_Y)]
    greeted += [(seq, lax.rem(tp + k, N_TP)) for k in range(1, N_TP)]
    for device in greeted:
        pl.semaphore_signal(barrier, inc=1, device_id=device, device_id_type=MESH)
    live_y[0] = jnp.full((8, 128), live_s[0], jnp.int32)
    block = lax.broadcasted_iota(jnp.int32, (8, 128), 1)
    place = jnp.zeros((8, 128), jnp.int32)
    for j in range(N_SEQ):
        place = jnp.where(block == owner_s[j], (j % 2) * (N_SEQ // 2) + j // 2, place)
    slot_v[...] = place
    gain_all = gain_v[...].astype(F32)
    gain_row = lax.broadcasted_iota(jnp.int32, (D // 128, 128), 0)
    gain = jnp.concatenate(
        [
            jnp.sum(jnp.where(gain_row == tp * 5 + i, gain_all, 0.0), axis=0, keepdims=True)
            for i in range(5)
        ],
        axis=1,
    )
    for load in loads:
        load.wait()
    own_a = rows[pl.ds(0, HALF), :].astype(F32)
    acts[tp, pl.ds(0, HALF), :] = (own_a * gain).astype(BF)
    row = lax.broadcasted_iota(jnp.int32, (HALF, CAP), 0)
    col = lax.broadcasted_iota(jnp.int32, (HALF, CAP), 1)
    chosen = (col == row + (live_s[0] - HALF)).astype(BF)
    tail_s[...] = jnp.dot(chosen, rows[...], preferred_element_type=F32).astype(BF)
    slots = pltpu.make_async_copy(slot_v, slot_s, local_sem.at[4])
    slots.start()
    pl.semaphore_wait(barrier, len(greeted))

    up_z = at_seq(y, wrap_z(zh + d), core)
    down_z = at_seq(y, wrap_z(zh - d), core)
    up_y = at_seq(wrap_y(y + d), zh, core)
    down_y = at_seq(wrap_y(y - d), zh, core)
    z_blocks = [zh, wrap_z(zh - d), wrap_z(zh + d), wrap_z(zh + 2 * d)]

    class Gather:
        def __init__(self, buf, first, count):
            self.buf, self.first, self.count = buf, first, count
            self.up, self.down, self.across = {}, {}, []

        def block(self, y_, z_):
            whole = self.count == BLK
            return self.buf.at[core, y_, z_] if whole else (
                self.buf.at[core, y_, z_, pl.ds(self.first, self.count)])

        def line_y(self, y_):
            whole = self.count == BLK
            return self.buf.at[core, y_] if whole else (
                self.buf.at[core, y_, :, pl.ds(self.first, self.count)])

        def line_z(self, z_):
            return self.buf.at[core, :, z_, pl.ds(self.first, self.count)]

        def z_own(self):
            own = self.block(y, zh)
            self.z1, self.z2 = send(own, own, up_z), send(own, own, down_z)

        def ring(self, b, k):
            if k > 1:
                self.up[b, k - 1].wait_recv()
            elif b == 1:
                self.z1.wait_recv()
                held = self.block(y, z_blocks[1])
                self.z3 = send(held, held, up_z)
            elif b == 2:
                self.z2.wait_recv()
            elif b == 3:
                self.z3.wait_recv()
            held = self.block(wrap_y(y - (k - 1) * d), z_blocks[b])
            self.up[b, k] = send(held, held, up_y)
            if k > 1:
                self.down[b, k - 1].wait_recv()
            if k < 4:
                held = self.block(wrap_y(y + (k - 1) * d), z_blocks[b])
                self.down[b, k] = send(held, held, down_y)

        def line_across(self, y_):
            held = self.line_y(wrap_y(y_))
            self.across.append(send(held, held, partner))

        def wave(self, w):
            for b, later in enumerate((0, 1, 1, 2)):
                if 1 <= w - later <= 4:
                    self.ring(b, w - later)
            if w == 3:
                self.line_across(y)
            elif w > 3:
                self.line_across(y - (w - 3) * d)
                self.line_across(y + (w - 3) * d)

        def last(self):
            for b in range(4):
                self.up[b, 4].wait_recv()
            self.line_across(y + 4)

        def column_own(self):
            own = self.line_z(zh)
            self.c1, self.c2 = send(own, own, up_z), send(own, own, down_z)
            self.across.append(send(own, own, partner))

        def column_on(self):
            self.c1.wait_recv()
            held = self.line_z(z_blocks[1])
            self.c3 = send(held, held, up_z)
            self.across.append(send(held, held, partner))

        def column_last(self):
            self.c2.wait_recv()
            held = self.line_z(z_blocks[2])
            self.across.append(send(held, held, partner))
            self.c3.wait_recv()
            held = self.line_z(z_blocks[3])
            self.across.append(send(held, held, partner))

        def wait(self):
            for copy in self.across:
                copy.wait_recv()

    kv = Gather(wkv, 0, BLK)
    qq = Gather(wq, 0, BLK)
    o1 = Gather(wo, 0, O_FIRST)
    o2 = Gather(wo, O_FIRST, BLK - O_FIRST)

    def squares(values):
        total = jnp.sum(values * values, axis=1, keepdims=True)
        return jnp.transpose(jnp.broadcast_to(total, (HALF, 128)))[:8]

    x_up = at_tp(wrap_x(x + 1), zl)
    x_down = at_tp(wrap_x(x - 1), zl)
    z_other = at_tp(x, 1 - zl)

    class Tokens:
        def __init__(self, part):
            self.part = part

        def chunk(self, x_, zl_):
            return acts.at[wrap_x(x_) * 2 + zl_, pl.ds(self.part * HALF, HALF)]

        def own(self):
            own = self.chunk(x, zl)
            self.a = [send(own, own, z_other), send(own, own, x_up), send(own, own, x_down)]

        def second(self):
            self.a[0].wait_recv()
            held = self.chunk(x, 1 - zl)
            self.b = [send(held, held, x_up), send(held, held, x_down)]

        def third(self):
            self.a[1].wait_recv()
            held = self.chunk(x - 1, zl)
            self.c = [send(held, held, x_up)]
            self.b[1].wait_recv()
            held = self.chunk(x + 1, 1 - zl)
            self.c.append(send(held, held, x_down))

        def wait(self):
            for copy in [self.a[2], self.b[0], *self.c]:
                copy.wait_recv()

    tok_a, tok_b = Tokens(0), Tokens(1)

    live_over_y = [
        send(live_y.at[0], live_y.at[k], at_seq(wrap_y(y + k), zh, core)) for k in range(1, N_Y)
    ]
    kv.z_own()
    kv.wave(1)
    qq.z_own()
    qq.wave(1)
    tok_a.own()
    o2.ring(0, 1)
    tail = send(tail_s, tail_r, next_1)
    ssq[tp, 0] = squares(own_a)

    position = seq * TOK + lax.broadcasted_iota(jnp.int32, (TOK, 128), 0)
    first = jnp.zeros((TOK, 128), jnp.int32)
    begin = docs_s[0]
    for doc in range(1, 32):
        first = jnp.maximum(first, jnp.where(position >= begin, begin, 0))
        begin = begin + docs_s[doc]
    key_base = [seq, seq - 2, seq - 3 + 2 * core, seq - 1 - 2 * core]
    lane = lax.broadcasted_iota(jnp.int32, (TOK, 128), 1)
    for b in range(4):
        for side in range(2):
            key_pos = key_base[b] * TOK + side * 128 + lane
            allowed = (key_pos <= position) & (key_pos >= first)
            bias[b, :, pl.ds(side * 128, 128)] = jnp.where(allowed, 0.0, NEG)

    kv.wave(2)
    for copy in live_over_y:
        copy.wait_recv()
    earlier = jnp.zeros((8, 128), jnp.int32)
    for k in range(1, N_Y):
        earlier = earlier + live_y[k] * (k <= y).astype(jnp.int32)
    live_c[0, 0] = earlier
    live_c[0, 1] = live_y[0]
    live_over_z = [
        send(
            live_c.at[0], live_c.at[n],
            at_seq(y, wrap_z(zh + n // 2), 1 - core if n % 2 else core),
        )
        for n in range(1, 2 * N_Z)
    ]
    o2.ring(0, 2)
    qq.wave(2)
    tok_a.second()
    kv.wave(3)
    o2.ring(0, 3)
    qq.wave(3)
    tok_a.third()
    o1.z_own()

    for copy in live_over_z:
        copy.wait_recv()
    before = live_c[0, 0] - seq * TOK
    for n in range(1, 2 * N_Z):
        counts = core if n == 1 else (n // 2 <= zh).astype(jnp.int32)
        before = before + live_c[n, 0] + live_c[n, 1] * counts
    spilled = before[:1, :]
    tail.wait_recv()
    row_b = lax.broadcasted_iota(jnp.int32, (HALF, 128), 0)
    keep = jnp.broadcast_to((row_b + spilled < HALF)[:, :1], (HALF, COLS))
    own_b = jnp.where(
        keep, rows[pl.ds(HALF, HALF), :].astype(F32), tail_r[...].astype(F32)
    )
    acts[tp, pl.ds(HALF, HALF), :] = (own_b * gain).astype(BF)
    tok_b.own()
    ssq[tp, 1] = squares(own_b)
    ssq_copies = [
        send(ssq.at[tp], ssq.at[tp], (seq, lax.rem(tp + k, N_TP))) for k in range(1, N_TP)
    ]
    kv.wave(4)
    o2.ring(0, 4)
    qq.wave(4)
    tok_b.second()
    o2.up[0, 4].wait_recv()
    o2.column_own()
    kv.wave(5)
    qq.wave(5)
    tok_b.third()
    o1.wave(1)
    o2.column_on()
    kv.wave(6)
    qq.wave(6)
    o1.wave(2)
    kv.last()
    o1.wave(3)

    def weight_of(buf, t):
        blocks = []
        for i in range(8):
            s = slot_s[0, t * 8 + i]
            blocks.append(
                buf[lax.div(s, N_Y * N_Z), lax.rem(lax.div(s, N_Z), N_Y), lax.rem(s, N_Z)]
            )
        return jnp.concatenate(blocks, axis=0)

    def project(buf, total):
        total[...] = jnp.zeros_like(total)

        def one(t, carry):
            total[...] += jnp.dot(acts[t], weight_of(buf, t), preferred_element_type=F32)
            return carry

        lax.fori_loop(0, N_TP, one, 0)

    slots.wait()
    tok_a.wait()
    tok_b.wait()
    for copy in ssq_copies:
        copy.wait_recv()
    kv.wait()
    project(wkv, acc_kv)

    total = ssq[0]
    for t in range(1, N_TP):
        total = total + ssq[t]
    scale_row = lax.rsqrt(total * (1.0 / D) + EPSILON)
    scale = jnp.concatenate(
        [jnp.transpose(jnp.broadcast_to(scale_row[h, :1], (128, 128))) for h in range(2)], axis=0
    )
    turn_row = lax.broadcasted_iota(jnp.int32, (TOK, TOK), 0)
    turn_col = lax.broadcasted_iota(jnp.int32, (TOK, TOK), 1)
    spilled_wide = jnp.concatenate([spilled, spilled], axis=1)
    turn = (((turn_col - turn_row + spilled_wide + TOK) & (TOK - 1)) == 0).astype(BF)

    def in_order(values):
        return jnp.dot(turn, values, preferred_element_type=F32).astype(BF)

    keys = in_order((acc_kv[:, :HD] * scale).astype(BF))
    values = in_order((acc_kv[:, HD:] * scale).astype(BF))
    kv_own[:, :HD] = keys
    kv_own[:, HD:] = values
    kv_1 = send(kv_own, kv_in.at[0], next_2)
    n_kv = len(started)

    def kv_copy(src):
        return pltpu.make_async_remote_copy(
            src_ref=src, dst_ref=kv_in.at[1], send_sem=send_sem.at[n_kv],
            recv_sem=recv_sem.at[n_kv], device_id=next_1, device_id_type=MESH,
        )

    @pl.when(core == 0)
    def _():
        kv_copy(kv_own).start()

    kv_2 = kv_copy(kv_own)
    started.append(kv_2)
    key_ref[...] = keys
    value_ref[...] = values
    qq.last()
    o1.wave(4)
    qq.wait()
    project(wq, acc_q)
    queries = [
        in_order((acc_q[:, h * HD : (h + 1) * HD] * scale * HD ** (-0.5)).astype(BF))
        for h in range(GROUP)
    ]
    o1.wave(5)
    kv_1.wait_recv()

    @pl.when(core == 1)
    def _():
        kv_copy(kv_in.at[0]).start()

    kv_3 = send(kv_in.at[0], kv_in.at[2], partner)
    o1.wave(6)
    o2.column_last()
    o1.last()
    kv_2.wait_recv()
    kv_3.wait_recv()

    pieces = [kv_own, kv_in.at[0], kv_in.at[1], kv_in.at[2]]
    for h in range(GROUP):
        scores = [
            lax.dot_general(
                queries[h], pieces[b][:, :HD], (((1,), (1,)), ((), ())),
                preferred_element_type=F32,
            ) + bias[b]
            for b in range(4)
        ]
        best = jnp.maximum(
            jnp.maximum(scores[0], scores[1]), jnp.maximum(scores[2], scores[3])
        )
        best = jnp.max(best, axis=1, keepdims=True)
        weights = [jnp.exp(s - best) for s in scores]
        totals = jnp.sum(weights[0] + weights[1] + weights[2] + weights[3], axis=1, keepdims=True)
        summed = jnp.dot(weights[0].astype(BF), pieces[0][:, HD:], preferred_element_type=F32)
        for b in range(1, 4):
            summed = summed + jnp.dot(
                weights[b].astype(BF), pieces[b][:, HD:], preferred_element_type=F32
            )
        ctx[:, h * HD : (h + 1) * HD] = (summed / totals).astype(BF)

    o1.wait()
    o2.wait()

    to_d = at_tp(wrap_x(x + d), zl)
    to_minus_d = at_tp(wrap_x(x - d), zl)
    x_order = [2, d, -d, 0]
    R2 = TOK - R1

    def partial_sum(j, side):
        t = wrap_x(x + x_order[j]) * 2 + (1 - zl if side == 0 else zl)
        part[j, side] = lax.dot_general(
            ctx[...], weight_of(wo, t), (((1,), (1,)), ((), ())), preferred_element_type=F32
        ).astype(BF)

    z1, relay2, direct2, sum2 = {}, {}, {}, {}
    for j in range(4):
        for side in range(2):
            partial_sum(j, side)
            rest = part.at[j, side, pl.ds(R1, R2)]
            if side == 0:
                z1[j] = send(part.at[j, 0, pl.ds(0, R1)], z1_r.at[j], z_other)
            if j == 0:
                relay2[side] = send(rest, x2_r.at[side, 0], to_d)
            if j == 2:
                direct2[side] = send(rest, x2_r.at[side, 1], to_minus_d)

    def rows_1(j):
        return part[j, 1, pl.ds(0, R1), :].astype(F32) + z1_r[j].astype(F32)

    def rows_2(j, side):
        return part[j, side, pl.ds(R1, R2), :].astype(F32)

    z1[0].wait_recv()
    pair_s[0] = rows_1(0).astype(BF)
    relay1 = send(pair_s.at[0], x1_r.at[0], to_d)
    for side in range(2):
        relay2[side].wait_recv()
        sum2_s[side] = (rows_2(1, side) + x2_r[side, 0].astype(F32)).astype(BF)
        sum2[side] = send(sum2_s.at[side], x2_r.at[side, 2], to_d)
    z1[1].wait_recv()
    z1[2].wait_recv()
    pair_s[2] = rows_1(2).astype(BF)
    direct1 = send(pair_s.at[2], x1_r.at[1], to_minus_d)
    relay1.wait_recv()
    pair_s[1] = (rows_1(1) + x1_r[0].astype(F32)).astype(BF)
    sum1 = send(pair_s.at[1], x1_r.at[2], to_d)

    def total_2(side):
        sum2[side].wait_recv()
        direct2[side].wait_recv()
        return rows_2(3, side) + x2_r[side, 1].astype(F32) + x2_r[side, 2].astype(F32)

    z2_s[...] = total_2(0).astype(BF)
    z2 = send(z2_s, z2_r, z_other)
    mine_2 = total_2(1)
    z1[3].wait_recv()
    direct1.wait_recv()
    sum1.wait_recv()
    out_ref[pl.ds(0, R1), :] = (
        rows_1(3) + x1_r[1].astype(F32) + x1_r[2].astype(F32)
    ).astype(BF)
    z2.wait_recv()
    out_ref[pl.ds(R1, R2), :] = (mine_2 + z2_r[...].astype(F32)).astype(BF)
    for copy in started:
        copy.wait_send()


def body(rollout_rows, live_rows, doc_lengths, block_owner, norm_gain, qkv_weight, out_weight):
    smem = pl.BlockSpec(memory_space=pltpu.SMEM)
    vmem = pl.BlockSpec(memory_space=pltpu.VMEM)
    anyw = pl.BlockSpec(memory_space=pl.ANY)
    V = pltpu.VMEM
    return pl.pallas_call(
        kernel,
        out_shape=(
            pltpu.VMEM((TOK, COLS), BF),
            pltpu.VMEM((TOK, HD), BF),
            pltpu.VMEM((TOK, HD), BF),
        ),
        in_specs=[smem, smem, smem, vmem, anyw, anyw, anyw],
        out_specs=(vmem, vmem, vmem),
        scratch_shapes=[
            V((CAP, COLS), BF),
            V((2, N_Y, N_Z, BLK, 2 * HD), BF),
            V((2, N_Y, N_Z, BLK, QW), BF),
            V((2, N_Y, N_Z, BLK, QW), BF),
            V((N_TP, TOK, COLS), BF),
            V((HALF, COLS), BF),
            V((HALF, COLS), BF),
            V((N_Y, 8, 128), jnp.int32),
            V((2 * N_Z, 2, 8, 128), jnp.int32),
            V((N_TP, 2, 8, 128), F32),
            V((8, 128), jnp.int32),
            pltpu.SMEM((8, 128), jnp.int32),
            V((TOK, 2 * HD), F32),
            V((TOK, QW), F32),
            V((TOK, 2 * HD), BF),
            V((3, TOK, 2 * HD), BF),
            V((4, TOK, TOK), F32),
            V((TOK, QW), BF),
            V((4, 2, TOK, COLS), BF),
            V((4, R1, COLS), BF),
            V((3, R1, COLS), BF),
            V((3, R1, COLS), BF),
            V((2, 3, TOK - R1, COLS), BF),
            V((2, TOK - R1, COLS), BF),
            V((TOK - R1, COLS), BF),
            V((TOK - R1, COLS), BF),
            pltpu.SemaphoreType.DMA((5,)),
            pltpu.SemaphoreType.DMA((N_COPIES,)),
            pltpu.SemaphoreType.DMA((N_COPIES,)),
        ],
        compiler_params=pltpu.CompilerParams(collective_id=0, has_side_effects=True),
    )(
        live_rows, doc_lengths, block_owner, norm_gain.reshape(D // 128, 128),
        rollout_rows, qkv_weight, out_weight,
    )


def solution(mesh):
    in_specs = (P("seq", "tp"), P("seq"), P(), P(), P(), P("seq", "tp"), P("seq", "tp"))
    out_specs = (P("seq", "tp"), P("seq", "tp"), P("seq", "tp"))
    return jax.shard_map(body, mesh=mesh, in_specs=in_specs, out_specs=out_specs, check_vma=False)
```
